256 devices in a mesh: theta: 16 (over y, z_hi, core), phi: 16 (over z_lo, x).
Axes of the slice: x: 4, y: 4, z: 8 (z_hi: 2, z_lo: 4; z = z_hi * 4 + z_lo), core: 2. Of those that a mesh axis runs over, the one named last changes fastest.
Arguments:
- fields: float32 [8, 2, 1024, 4096], P(None, None, 'theta', 'phi'), may hold values from -6 to 6
- legendre: float32 [1024, 512, 1025], P('theta', 'phi'), may hold values from -0.0029296875 to 0.0029296875
- pair_table: int32 [512], replicated, may hold values from 0 to 511, each once
Outputs:
- coefficients: float32 [512, 2, 8, 1025], P(('phi', 'theta'))
The draws below stay inside these ranges and needn't reach their ends.
Inputs may be any that keep to these rules, and one draw needn't show every extreme that they name: A permutation: slot s holds the orders 1024 + pair_table[s] and 2047 - pair_table[s].
All inputs are finite; a program needn't handle non-finite values.
Results may differ from the reference program's by a relative error of at most 0.0003.
Values sent between devices are 32-bit elements; how exact they have to be, the bound alone decides.
A program may use at most 64 MiB of HBM per device.

```python
import jax
import jax.numpy as jnp
from jax import lax

LATS = 2048
HALF_LATS = 1024
LONS = 4096
DEGREES = 2048
ORDERS = 1024
LOW_ORDER = 1024
PAIRS = 512
PAIR_LEN = 1025
FIELDS = 8


def spiked(array, stream_key, source, target, shards_of, factor):
    def block_of(axis_at):
        return (jnp.arange(array.shape[axis_at]) // (array.shape[axis_at] // shards_of)).reshape((-1,) + (1,) * (array.ndim - 1 - axis_at))

    one_side = jax.random.permutation(stream_key, shards_of)[block_of(target)]
    second = (block_of(target) + shards_of // 2) % shards_of
    return jnp.where((block_of(source) == one_side) | (block_of(source) == second), factor * array, array)


def level_of(key, extent, cuts, smallest, largest):
    def one(dim, shards_of):
        draws = jax.random.uniform(jax.random.fold_in(jax.random.fold_in(key, 6), dim), (shards_of,), jnp.float32, smallest / len(cuts), largest / len(cuts))
        return jnp.repeat(jnp.exp(draws), extent[dim] // shards_of).reshape((-1,) + (1,) * (len(extent) - dim - 1))

    level = one(*cuts[0])
    for cut in cuts[1:]:
        level = level * one(*cut)
    return level


def normal_values(own_key, shape, scale, bound, cuts=(), held_as=jnp.bfloat16):
    array = jax.random.normal(own_key, shape, jnp.float32) * scale
    if len(cuts) > 0:
        array = level_of(own_key, shape, cuts, -0.22, 0.18) * array
    return jnp.clip(array, min=-bound, max=bound).astype(held_as)


def bell_draw_with(key, extent, spread, reach, shards, heavy, kind=jnp.bfloat16):
    entries = spread * jax.random.normal(key, extent, jnp.float32)
    if shards:
        entries = entries * level_of(key, extent, shards, -0.22, 0.18)
    return jnp.clip(spiked(entries, jax.random.fold_in(key, 3), *heavy), -reach, reach).astype(kind)


def setup_inputs(seed: int = 0) -> dict:
    arg_keys = jax.random.split(jax.random.key(seed), 4)
    return {
        "fields": normal_values(arg_keys[0], (FIELDS, 2, HALF_LATS, LONS), 1.0, 6.0, ((2, 16), (3, 16)), jnp.float32),
        "legendre": bell_draw_with(arg_keys[1], (HALF_LATS, PAIRS, PAIR_LEN), (LONS * LATS) ** -0.5, 0.0029296875, ((0, 16), (1, 16)), (0, 1, 16, 2.0), jnp.float32),
        "pair_table": jax.random.permutation(arg_keys[2], PAIRS).astype(jnp.int32),
    }


full_precision = lax.Precision.HIGHEST


def reference(fields, legendre, pair_table):
    spectrum = jnp.fft.rfft(fields, axis=-1)[..., LOW_ORDER:DEGREES]
    window = jnp.stack([jnp.real(spectrum), jnp.imag(spectrum)], axis=0).astype(jnp.float32)
    even = window[:, :, 0] + window[:, :, 1]
    odd = window[:, :, 0] - window[:, :, 1]
    columns = jnp.arange(PAIR_LEN, dtype=jnp.int32)

    def take(values, index):
        return lax.dynamic_index_in_dim(values, index, axis=3, keepdims=False)

    def one_slot(slot):
        pair = pair_table[slot]
        weights = lax.dynamic_index_in_dim(legendre, slot, axis=1, keepdims=False)
        first = columns < ORDERS - pair
        parity = jnp.where(first, columns % 2, (columns + pair) % 2)
        upper = ORDERS - 1 - pair

        def project(values):
            return jnp.einsum("rfj,jc->rfc", values, weights, precision=full_precision)

        even_first = project(take(even, pair))
        odd_first = project(take(odd, pair))
        even_second = project(take(even, upper))
        odd_second = project(take(odd, upper))
        lower_part = jnp.where(parity == 0, even_first, odd_first)
        upper_part = jnp.where(parity == 0, even_second, odd_second)
        return jnp.where(first, lower_part, upper_part)

    return lax.map(one_slot, jnp.arange(PAIRS, dtype=jnp.int32))
```

```python
import math

import jax
import jax.numpy as jnp
import numpy as np
from jax import lax
from jax.sharding import PartitionSpec as P

LONS = 4096
DEGREES = 2048
ORDERS = 1024
LOW_ORDER = 1024
PAIR_LEN = 1025

HIGH = lax.Precision.HIGH


def dft_tables():
    r = np.arange(16)
    k = np.arange(256)
    twiddle = 2.0 * np.pi * np.outer(r, k) / LONS
    a = np.arange(32)
    m1 = np.concatenate([64 + a, 127 - a])
    inner = 2.0 * np.pi * (np.outer(m1, k) % 256) / 256
    outer = 2.0 * np.pi * (np.outer(r, r) % 16) / 16
    return [np.stack([np.cos(t), np.sin(t)]).astype(np.float32) for t in (outer, twiddle, inner)]


def orders_of(rows):
    outer, twiddle, inner = dft_tables()
    y = jnp.einsum("zrp,pjk->zrjk", jnp.asarray(outer), rows, precision=HIGH)
    y_re, y_im = y[0], -y[1]
    c, s = jnp.asarray(twiddle)[:, :, None, :]
    z_re = y_re * c + y_im * s
    z_im = y_im * c - y_re * s
    cos, sin = inner
    both = np.stack([np.concatenate([cos, sin], 1), np.concatenate([-sin, cos], 1)])
    z = jnp.concatenate([z_re, z_im], axis=-1)
    x = jnp.einsum("znk,rjk->nrzj", jnp.asarray(both), z, precision=HIGH)
    first = x[:32].reshape(512, 2, -1)
    second = x[32:, ::-1].reshape(512, 2, -1)
    return jnp.stack([first, second])


def order_masks(pairs):
    columns = jnp.arange(PAIR_LEN, dtype=jnp.int32)[None, :]
    shifts = pairs[:, None]
    first = columns < ORDERS - shifts
    even = jnp.where(first, columns % 2, (columns + shifts) % 2) == 0
    return first[:, None, :], even[:, None, :]


def on_device(fields, legendre, pair_table):
    phi_index = lax.axis_index("phi")
    theta = lax.axis_index("theta")
    slots = legendre.shape[1]
    own_pairs = lax.dynamic_slice_in_dim(pair_table, phi_index * slots, slots)
    rows = jnp.swapaxes(fields, 0, 1).reshape(16, 64, 256)
    rows = lax.all_to_all(rows, "phi", 0, 0, tiled=True)
    x = orders_of(rows)
    x = jnp.take(x, pair_table, axis=1).reshape(2, 16, 32, 128)
    x = jnp.swapaxes(x, 0, 1)
    x = lax.all_to_all(x, "phi", 0, 0, tiled=True)
    v = x.reshape(2, 8, 2, 32, 2, 64)
    even, odd = v[0] + v[1], v[0] - v[1]
    v = jnp.stack([even, odd])
    v = v.transpose(3, 2, 0, 4, 1, 5).reshape(32, 64, 64)
    out = lax.dot_general(v, legendre, (((2,), (0,)), ((0,), (1,))), precision=HIGH)
    out = out.reshape(32, 2, 2, 16, PAIR_LEN)
    first, even = order_masks(own_pairs)
    lower = jnp.where(even, out[:, 0, 0], out[:, 0, 1])
    upper = jnp.where(even, out[:, 1, 0], out[:, 1, 1])
    part = jnp.where(first, lower, upper).reshape(4, 2, 2, 2, 16, PAIR_LEN)
    core = theta % 2
    mine = jnp.take(part, core, axis=2)
    other = jnp.take(part, 1 - core, axis=2)
    got = lax.ppermute(other, "theta", [(i, i ^ 1) for i in range(16)])
    part = mine + got
    groups = [[y * 4 + i for y in range(4)] for i in range(4)]
    part = lax.all_to_all(part, "theta", 0, 0, axis_index_groups=groups, tiled=True).sum(axis=0)
    z = (theta // 2) % 2
    mine = jnp.take(part, z, axis=0)
    other = jnp.take(part, 1 - z, axis=0)
    got = lax.ppermute(other, "theta", [(i, i ^ 2) for i in range(16)])
    return (mine + got).reshape(2, 2, 8, PAIR_LEN)


def solution(mesh):
    placed = (P(None, None, "theta", "phi"), P("theta", "phi", None), P())
    return jax.shard_map(
        on_device,
        mesh=mesh,
        in_specs=placed,
        out_specs=P(("phi", "theta"), None, None, None),
        check_vma=False,
    )
```

```python
import functools
import math

import jax
import jax.numpy as jnp
import numpy as np
from jax import lax
from jax.experimental import pallas as pl
from jax.experimental.pallas import tpu as pltpu
from jax.sharding import PartitionSpec as P

LONS = 4096
ORDERS = 1024
PAIR_LEN = 1025

MESH = pl.DeviceIdType.MESH
F32 = jnp.float32
BF16 = jnp.bfloat16


def dft_tables():
    r = np.arange(16)
    k = np.arange(256)
    twiddle = 2.0 * np.pi * np.outer(r, k) / LONS
    a = np.arange(32)
    m1 = np.concatenate([64 + a, 127 - a])
    inner = 2.0 * np.pi * (np.outer(m1, k) % 256) / 256
    cos, sin = np.cos(inner), np.sin(inner)
    both = np.concatenate([np.concatenate([cos, sin], 1), np.concatenate([-sin, cos], 1)])
    both = both.astype(np.float32)
    high = both.astype(BF16)
    low = (both - high.astype(np.float32)).astype(BF16)
    return np.stack([np.cos(twiddle), np.sin(twiddle)]).astype(np.float32), high, low


def halves(x):
    high = x.astype(BF16)
    return high, (x - high.astype(F32)).astype(BF16)


def weighted(terms):
    total = None
    for weight, value in terms:
        if abs(weight) < 1e-12:
            continue
        if abs(weight - 1.0) < 1e-12:
            total = value if total is None else total + value
        elif abs(weight + 1.0) < 1e-12:
            total = -value if total is None else total - value
        else:
            total = value * weight if total is None else total + value * weight
    return total


def sixteen_point(x):
    e = [None] + [x[j] + x[16 - j] for j in range(1, 8)]
    o = [None] + [x[j] - x[16 - j] for j in range(1, 8)]
    cos = lambda t: math.cos(math.pi * t / 8)
    sin = lambda t: math.sin(math.pi * t / 8)
    base = [x[0] + x[8], x[0] - x[8]]
    re_of, im_of = [], []
    plus_e = [e[j] + e[8 - j] for j in range(1, 4)]
    less_e = [e[j] - e[8 - j] for j in range(1, 4)]
    plus_o = [o[j] + o[8 - j] for j in range(1, 4)]
    less_o = [o[j] - o[8 - j] for j in range(1, 4)]
    for r in range(9):
        fold_e, fold_o = (less_e, plus_o) if r % 2 else (plus_e, less_o)
        re_terms = [(1.0, base[r % 2])] + [(cos(j * r), fold_e[j - 1]) for j in (1, 2, 3)]
        im_terms = [(-sin(j * r), fold_o[j - 1]) for j in (1, 2, 3)]
        if r % 2:
            im_terms.append((-sin(4 * r), o[4]))
        else:
            re_terms.append((cos(4 * r), e[4]))
        re_of.append(weighted(re_terms))
        im_of.append(weighted(im_terms))
    return re_of, im_of


def dot(a, b):
    return lax.dot_general(a, b, (((1,), (0,)), ((), ())), preferred_element_type=F32)


def dot_rows(a, b):
    return lax.dot_general(a, b, (((1,), (1,)), ((), ())), preferred_element_type=F32)


def kernel(
    fields, legendre, pairs, pair_scalars, twiddle, inner_high, inner_low, out,
    staged, weights, rows, z_high, z_low, a_high, a_low, chosen, ordered, arrived,
    part, from_core, ring_in, near_in, joined, joined_in, whole, from_far,
    leg_sem, s1, r1, s2, r2, sa, ra, sb, rb, sc, rc, sz, rz,
):
    theta = lax.axis_index("theta")
    phi = lax.axis_index("phi")
    z, x = phi // 4, phi % 4
    y, far, core = theta // 4, (theta // 2) % 2, theta % 2
    core_mate = theta + 1 - 2 * core
    far_mate = theta + 2 - 4 * far
    up = ((y + 1) % 4) * 4 + theta % 4
    down = ((y + 3) % 4) * 4 + theta % 4

    loads = [
        pltpu.make_async_copy(legendre.at[pl.ds(16 * c, 16)], staged.at[pl.ds(16 * c, 16)], leg_sem.at[c])
        for c in range(4)
    ]
    for load in loads:
        load.start()

    z_order = [(z + 2) % 4, 3 - z, z + 1 - 2 * (z % 2), z]
    partners = []
    for step, other_z in enumerate(z_order):
        for dx in range(4):
            if step == 3 and dx == 0:
                continue
            partners.append(other_z * 4 + (x + dx) % 4)

    barrier = pltpu.get_barrier_semaphore()
    for partner in partners:
        pl.semaphore_signal(barrier, inc=1, device_id=(theta, partner), device_id_type=MESH)
    for partner in (core_mate, far_mate, up, down):
        pl.semaphore_signal(barrier, inc=1, device_id=(partner, phi), device_id_type=MESH)
    pl.semaphore_wait(barrier, 19)

    def send(src, dst, send_sem, recv_sem, device):
        copy = pltpu.make_async_remote_copy(
            src_ref=src, dst_ref=dst, send_sem=send_sem, recv_sem=recv_sem, device_id=device, device_id_type=MESH
        )
        return copy

    first_sends = []
    for n, partner in enumerate(partners):
        copy = send(fields.at[partner % 8, partner // 8], rows.at[phi], s1.at[n], r1.at[phi], (theta, partner))
        copy.start()
        first_sends.append(copy)
    rows[phi] = fields[phi % 8, phi // 8]

    spread = jnp.broadcast_to(pairs[...].astype(F32), (128, 512))
    lane = lax.broadcasted_iota(jnp.int32, (128, 128), 1)
    for block in range(4):
        own = jnp.transpose(spread[:, 128 * block : 128 * block + 128])
        for tile in range(4):
            code = (16 * (lane % 32) + (4 * tile + lane // 32)).astype(F32)
            chosen[128 * block : 128 * block + 128, 128 * tile : 128 * tile + 128] = jnp.where(
                own == code, 1.0, 0.0
            ).astype(BF16)

    for load in loads:
        load.wait()

    def prepare(n, carry):
        lat, slot = 16 * (n // 4), 8 * (n % 4)
        for tile in range(9):
            lanes = slice(128 * tile, min(128 * tile + 128, PAIR_LEN))
            block = staged[pl.ds(lat, 16), pl.ds(slot, 8), lanes]
            high, low = halves(jnp.transpose(block, (1, 0, 2)))
            weights[pl.ds(slot, 8), pl.ds(lat, 16), lanes] = high
            weights[pl.ds(slot, 8), pl.ds(64 + lat, 16), lanes] = high
            weights[pl.ds(slot, 8), pl.ds(128 + lat, 16), lanes] = low
        return carry

    lax.fori_loop(0, 16, prepare, 0)

    for partner in partners:
        send(rows.at[partner], rows.at[partner], s1.at[0], r1.at[partner], (theta, partner)).wait_recv()

    def outer(n, carry):
        lat = 16 * (n // 2)
        lanes = pl.ds(pl.multiple_of(128 * (n % 2), 128), 128)
        upper = pl.ds(pl.multiple_of(256 + 128 * (n % 2), 128), 128)
        re_of, im_of = sixteen_point([rows[p, pl.ds(lat, 16), lanes] for p in range(16)])
        for r in range(16):
            re = re_of[min(r, 16 - r)]
            im = im_of[min(r, 16 - r)]
            c = twiddle[0, r : r + 1, lanes]
            s = twiddle[1, r : r + 1, lanes]
            if im is None:
                z_re, z_im = re * c, -(re * s)
            elif r <= 8:
                z_re, z_im = re * c + im * s, im * c - re * s
            else:
                z_re, z_im = re * c - im * s, -(im * c + re * s)
            for value, at in ((z_re, lanes), (z_im, upper)):
                high, low = halves(value)
                z_high[r, pl.ds(lat, 16), at] = high
                z_low[r, pl.ds(lat, 16), at] = low
        return carry

    lax.fori_loop(0, 8, outer, 0)

    def inner(r, carry):
        high, low = z_high[r], z_low[r]
        both = dot_rows(inner_high[...], high) + dot_rows(inner_high[...], low) + dot_rows(inner_low[...], high)
        for kind, at in ((0, r), (1, 15 - r)):
            value = jnp.concatenate([both[32 * kind : 32 * kind + 32], both[64 + 32 * kind : 96 + 32 * kind]], axis=1)
            high_value, low_value = halves(value)
            lanes = slice(128 * kind, 128 * kind + 128)
            spot = pl.ds(pl.multiple_of(32 * at, 32), 32)
            a_high[spot, lanes] = high_value
            a_low[spot, lanes] = low_value
        return carry

    lax.fori_loop(0, 16, inner, 0)

    second_sends = []
    for step, other_z in enumerate(z_order):
        at = pl.ds(pl.multiple_of(128 * other_z, 128), 128)
        picks = chosen[at, :]
        value = dot(picks, a_high[...]) + dot(picks, a_low[...])
        ordered[0, at, :] = value[:, :128]
        ordered[1, at, :] = value[:, 128:]
        for dx in range(4):
            if step == 3 and dx == 0:
                continue
            n = 4 * step + dx - (1 if step == 3 else 0)
            partner = partners[n]
            copy = send(
                ordered.at[:, pl.ds(pl.multiple_of(32 * partner, 32), 32), :],
                arrived.at[:, pl.ds(pl.multiple_of(32 * phi, 32), 32), :],
                s2.at[n],
                r2.at[phi],
                (theta, partner),
            )
            copy.start()
            second_sends.append(copy)
    mine = pl.ds(pl.multiple_of(32 * phi, 32), 32)
    arrived[:, mine, :] = ordered[:, mine, :]

    for partner in partners:
        spot = arrived.at[:, pl.ds(pl.multiple_of(32 * partner, 32), 32), :]
        send(spot, spot, s2.at[0], r2.at[partner], (theta, partner)).wait_recv()

    column = lax.broadcasted_iota(jnp.int32, (8, PAIR_LEN), 1)

    def project(slot, at):
        rows_of = []
        for kind in range(2):
            both = arrived[kind, pl.ds(slot, 16, stride=32), :]
            rows_of += [both[:8] + both[8:], both[:8] - both[8:]]
        value = jnp.concatenate(rows_of, axis=0)
        value = jnp.concatenate([value[:, :64], value[:, 64:]], axis=0)
        high = value.astype(BF16).astype(F32)
        left = jnp.concatenate([high, value - high, high], axis=1).astype(BF16)
        product = dot(left, weights[slot])
        pair = pair_scalars[32 * phi + slot]
        is_first = column < ORDERS - pair
        is_even = (column + jnp.where(is_first, 0, pair)) % 2 == 0
        for half in range(2):
            four = [product[32 * half + 8 * n : 32 * half + 8 * n + 8] for n in range(4)]
            lower = jnp.where(is_even, four[0], four[1])
            upper = jnp.where(is_even, four[2], four[3])
            part[at, 8 * half : 8 * half + 8, :] = jnp.where(is_first, lower, upper)

    def project_half(e, of_core):
        def body(n, carry):
            project(8 * (n // 2) + 4 * (n % 2) + 2 * of_core + e, 16 * e + 8 * of_core + n)
            return carry

        lax.fori_loop(0, 8, body, 0)

    core_sends, ring_sends = [], []
    for e in range(2):
        project_half(e, 1 - core)
        copy = send(
            part.at[pl.ds(16 * e + 8 * (1 - core), 8)], from_core.at[e], sa.at[e], ra.at[e], (core_mate, phi)
        )
        copy.start()
        core_sends.append(copy)
        project_half(e, core)

    def own(e, to_y, half):
        return 16 * e + 8 * core + 2 * to_y + half

    y_up, y_down, y_far = (y + 1) % 4, (y + 3) % 4, (y + 2) % 4
    near_sends = []
    for e in range(2):
        core_sends[e].wait_recv()
        mine_at = pl.ds(16 * e + 8 * core, 8)
        part[mine_at] = part[mine_at] + from_core[e]
        for n, (src, dst, device) in enumerate((
            (own(e, y_far, 0), ring_in.at[e, 0], up),
            (own(e, y_far, 1), ring_in.at[e, 1], down),
            (own(e, y_up, 1), near_in.at[e, 0], up),
            (own(e, y_down, 0), near_in.at[e, 1], down),
        )):
            copy = send(part.at[src], dst, sb.at[e, n], rb.at[e, n], (device, phi))
            copy.start()
            near_sends.append(copy)

    joined_sends = []
    for e in range(2):
        for n, (src, device) in enumerate(((own(e, y_up, 0), up), (own(e, y_down, 1), down))):
            near_sends[4 * e + n].wait_recv()
            joined[e, n] = part[src] + ring_in[e, n]
            copy = send(joined.at[e, n], joined_in.at[e, n], sc.at[e, n], rc.at[e, n], (device, phi))
            copy.start()
            joined_sends.append(copy)

    far_sends = []
    for e in range(2):
        near_sends[4 * e + 2].wait_recv()
        near_sends[4 * e + 3].wait_recv()
        joined_sends[2 * e].wait_recv()
        joined_sends[2 * e + 1].wait_recv()
        whole[e, 0] = part[own(e, y, 0)] + joined_in[e, 0] + near_in[e, 1]
        whole[e, 1] = part[own(e, y, 1)] + joined_in[e, 1] + near_in[e, 0]
        copy = send(whole.at[e, 1 - far], from_far.at[e], sz.at[e], rz.at[e], (far_mate, phi))
        copy.start()
        far_sends.append(copy)
    for e in range(2):
        far_sends[e].wait_recv()
        out[e] = whole[e, far] + from_far[e]

    for copy in first_sends + second_sends + core_sends + near_sends + joined_sends + far_sends:
        copy.wait_send()


def on_device(fields, legendre, pair_table):
    twiddle, inner_high, inner_low = dft_tables()
    vmem = pl.BlockSpec(memory_space=pltpu.VMEM)
    dma = pltpu.SemaphoreType.DMA
    row = (16, PAIR_LEN)
    result = pl.pallas_call(
        kernel,
        out_shape=jax.ShapeDtypeStruct((2, *row), F32),
        in_specs=[
            vmem,
            pl.BlockSpec(memory_space=pl.ANY),
            vmem,
            pl.BlockSpec(memory_space=pltpu.SMEM),
            vmem,
            vmem,
            vmem,
        ],
        out_specs=vmem,
        scratch_shapes=[
            pltpu.VMEM((64, 32, PAIR_LEN), F32),
            pltpu.VMEM((32, 192, PAIR_LEN), BF16),
            pltpu.VMEM((16, 64, 256), F32),
            pltpu.VMEM((16, 64, 512), BF16),
            pltpu.VMEM((16, 64, 512), BF16),
            pltpu.VMEM((512, 256), BF16),
            pltpu.VMEM((512, 256), BF16),
            pltpu.VMEM((512, 512), BF16),
            pltpu.VMEM((2, 512, 128), F32),
            pltpu.VMEM((2, 512, 128), F32),
            pltpu.VMEM((32, *row), F32),
            pltpu.VMEM((2, 8, *row), F32),
            pltpu.VMEM((2, 2, *row), F32),
            pltpu.VMEM((2, 2, *row), F32),
            pltpu.VMEM((2, 2, *row), F32),
            pltpu.VMEM((2, 2, *row), F32),
            pltpu.VMEM((2, 2, *row), F32),
            pltpu.VMEM((2, *row), F32),
            dma((4,)),
            dma((15,)), dma((16,)),
            dma((15,)), dma((16,)),
            dma((2,)), dma((2,)),
            dma((2, 4)), dma((2, 4)),
            dma((2, 2)), dma((2, 2)),
            dma((2,)), dma((2,)),
        ],
        compiler_params=pltpu.CompilerParams(
            collective_id=0, has_side_effects=True, vmem_limit_bytes=60 * 1024 * 1024
        ),
        name="harmonics",
    )(
        fields,
        legendre,
        pair_table.reshape(1, -1),
        pair_table,
        jnp.asarray(twiddle),
        jnp.asarray(inner_high),
        jnp.asarray(inner_low),
    )
    return result.reshape(2, 2, 8, PAIR_LEN)


def solution(mesh):
    placed = (P(None, None, "theta", "phi"), P("theta", "phi", None), P())
    return jax.shard_map(
        on_device,
        mesh=mesh,
        in_specs=placed,
        out_specs=P(("phi", "theta"), None, None, None),
        check_vma=False,
    )
```

```python
import functools
import math

import jax
import jax.numpy as jnp
import numpy as np
from jax import lax
from jax.experimental import pallas as pl
from jax.experimental.pallas import tpu as pltpu
from jax.sharding import PartitionSpec as P

LONS = 4096
ORDERS = 1024
PAIR_LEN = 1025

MESH = pl.DeviceIdType.MESH
F32 = jnp.float32
BF16 = jnp.bfloat16


def dft_tables():
    r = np.arange(16)
    k = np.arange(256)
    twiddle = 2.0 * np.pi * np.outer(r, k) / LONS
    a = np.arange(32)
    m1 = np.concatenate([64 + a, 127 - a])
    inner = 2.0 * np.pi * (np.outer(m1, k) % 256) / 256
    cos, sin = np.cos(inner), np.sin(inner)
    both = np.stack([np.concatenate([cos, sin], 1), np.concatenate([-sin, cos], 1)])
    both = both.reshape(2, 2, 32, 512).transpose(1, 0, 2, 3).reshape(128, 512)
    both = both.astype(np.float32)
    high = both.astype(BF16)
    low = (both - high.astype(np.float32)).astype(BF16)
    return np.stack([np.cos(twiddle), np.sin(twiddle)]).astype(np.float32), high, low


def halves(x):
    high = x.astype(BF16)
    return high, (x - high.astype(F32)).astype(BF16)


def weighted(terms):
    total = None
    for weight, value in terms:
        if abs(weight) < 1e-12:
            continue
        if abs(weight - 1.0) < 1e-12:
            total = value if total is None else total + value
        elif abs(weight + 1.0) < 1e-12:
            total = -value if total is None else total - value
        else:
            total = value * weight if total is None else total + value * weight
    return total


def sixteen_point(x):
    e = [None] + [x[j] + x[16 - j] for j in range(1, 8)]
    o = [None] + [x[j] - x[16 - j] for j in range(1, 8)]
    cos = lambda t: math.cos(math.pi * t / 8)
    sin = lambda t: math.sin(math.pi * t / 8)
    base = [x[0] + x[8], x[0] - x[8]]
    re_of, im_of = [], []
    plus_e = [e[j] + e[8 - j] for j in range(1, 4)]
    less_e = [e[j] - e[8 - j] for j in range(1, 4)]
    plus_o = [o[j] + o[8 - j] for j in range(1, 4)]
    less_o = [o[j] - o[8 - j] for j in range(1, 4)]
    for r in range(9):
        fold_e, fold_o = (less_e, plus_o) if r % 2 else (plus_e, less_o)
        re_terms = [(1.0, base[r % 2])] + [(cos(j * r), fold_e[j - 1]) for j in (1, 2, 3)]
        im_terms = [(-sin(j * r), fold_o[j - 1]) for j in (1, 2, 3)]
        if r % 2:
            im_terms.append((-sin(4 * r), o[4]))
        else:
            re_terms.append((cos(4 * r), e[4]))
        re_of.append(weighted(re_terms))
        im_of.append(weighted(im_terms))
    return re_of, im_of


def dot(a, b):
    return lax.dot_general(a, b, (((1,), (0,)), ((), ())), preferred_element_type=F32)


def dot_rows(a, b):
    return lax.dot_general(a, b, (((1,), (1,)), ((), ())), preferred_element_type=F32)


def kernel(
    fields, legendre, pairs, pair_scalars, twiddle, inner_high, inner_low, out,
    staged, weights, rows, z_high, z_low, a_high, a_low, spread_pairs, chosen, ordered, arrived,
    left, part, from_core, ring_in, near_in, joined, joined_in, whole, from_far,
    leg_sem, s1, r1, s2, r2, sa, ra, sb, rb, sc, rc, sz, rz,
):
    theta = lax.axis_index("theta")
    phi = lax.axis_index("phi")
    z, x = phi // 4, phi % 4
    y, far, core = theta // 4, (theta // 2) % 2, theta % 2
    core_mate = theta + 1 - 2 * core
    far_mate = theta + 2 - 4 * far
    up = ((y + 1) % 4) * 4 + theta % 4
    down = ((y + 3) % 4) * 4 + theta % 4

    loads = [
        pltpu.make_async_copy(legendre.at[pl.ds(16 * c, 16)], staged.at[pl.ds(16 * c, 16)], leg_sem.at[c])
        for c in range(4)
    ]
    for load in loads:
        load.start()

    z_order = [(z + 2) % 4, 3 - z, z + 1 - 2 * (z % 2), z]
    partners = []
    for step, other_z in enumerate(z_order):
        for dx in range(4):
            if step == 3 and dx == 0:
                continue
            partners.append(other_z * 4 + (x + dx) % 4)

    barrier = pltpu.get_barrier_semaphore()
    for partner in partners:
        pl.semaphore_signal(barrier, inc=1, device_id=(theta, partner), device_id_type=MESH)
    for partner in (core_mate, far_mate, up, down):
        pl.semaphore_signal(barrier, inc=1, device_id=(partner, phi), device_id_type=MESH)
    pl.semaphore_wait(barrier, 19)

    def send(src, dst, send_sem, recv_sem, device):
        return pltpu.make_async_remote_copy(
            src_ref=src, dst_ref=dst, send_sem=send_sem, recv_sem=recv_sem, device_id=device, device_id_type=MESH
        )

    sent = []

    def start(*copy_args):
        copy = send(*copy_args)
        copy.start()
        sent.append(copy)
        return copy

    for h in range(2):
        lats = pl.ds(32 * h, 32)
        for n, partner in enumerate(partners):
            start(
                fields.at[partner % 8, partner // 8, lats],
                rows.at[h, phi],
                s1.at[h, n],
                r1.at[h, phi],
                (theta, partner),
            )
        rows[h, phi] = fields[phi % 8, phi // 8, lats]

    spread = jnp.broadcast_to(pairs[...].astype(F32), (128, 512))
    for block in range(4):
        at = slice(128 * block, 128 * block + 128)
        spread_pairs[at, :] = jnp.transpose(spread[:, at])
    lane = lax.broadcasted_iota(jnp.int32, (128, 128), 1)
    for e in range(2):
        for block in range(2):
            own = spread_pairs[pl.ds(256 * block + e, 128, stride=2), :]
            for tile in range(4):
                code = (16 * (lane % 32) + (4 * tile + lane // 32)).astype(F32)
                chosen[e, 128 * block : 128 * block + 128, 128 * tile : 128 * tile + 128] = jnp.where(
                    own == code, 1.0, 0.0
                ).astype(BF16)

    def prepare(n, carry):
        lat, slot = 16 * (n // 4), 8 * (n % 4)
        for tile in range(9):
            lanes = slice(128 * tile, min(128 * tile + 128, PAIR_LEN))
            block = staged[pl.ds(lat, 16), pl.ds(slot, 8), lanes]
            high, low = halves(jnp.transpose(block, (1, 0, 2)))
            weights[pl.ds(slot, 8), pl.ds(lat, 16), lanes] = high
            weights[pl.ds(slot, 8), pl.ds(64 + lat, 16), lanes] = high
            weights[pl.ds(slot, 8), pl.ds(128 + lat, 16), lanes] = low
        return carry

    def outer(h):
        def body(n, carry):
            lat = pl.multiple_of(16 * (n // 2), 16)
            lanes = pl.ds(pl.multiple_of(128 * (n % 2), 128), 128)
            upper = pl.ds(pl.multiple_of(256 + 128 * (n % 2), 128), 128)
            re_of, im_of = sixteen_point([rows[h, p, pl.ds(lat, 16), lanes] for p in range(16)])
            for r in range(16):
                re = re_of[min(r, 16 - r)]
                im = im_of[min(r, 16 - r)]
                c = twiddle[0, r : r + 1, lanes]
                s = twiddle[1, r : r + 1, lanes]
                if im is None:
                    z_re, z_im = re * c, -(re * s)
                elif r <= 8:
                    z_re, z_im = re * c + im * s, im * c - re * s
                else:
                    z_re, z_im = re * c - im * s, -(im * c + re * s)
                for value, at in ((z_re, lanes), (z_im, upper)):
                    high, low = halves(value)
                    z_high[pl.ds(32 * r + lat, 16), at] = high
                    z_low[pl.ds(32 * r + lat, 16), at] = low
            return carry

        lax.fori_loop(0, 4, body, 0)

    def inner():
        for group in range(4):
            at = slice(128 * group, 128 * group + 128)
            high, low = z_high[at, :], z_low[at, :]
            both = dot_rows(inner_high[...], high) + dot_rows(inner_high[...], low) + dot_rows(inner_low[...], high)
            for j in range(4):
                lats = slice(32 * j, 32 * j + 32)
                r = 4 * group + j
                for kind, spot in ((0, r), (1, 15 - r)):
                    value = jnp.concatenate(
                        [both[64 * kind : 64 * kind + 32, lats], both[64 * kind + 32 : 64 * kind + 64, lats]], axis=1
                    )
                    high_value, low_value = halves(value)
                    a_high[32 * spot : 32 * spot + 32, 64 * kind : 64 * kind + 64] = high_value
                    a_low[32 * spot : 32 * spot + 32, 64 * kind : 64 * kind + 64] = low_value

    def order_and_send(h):
        for e in range(2):
            picks = chosen[e]
            ordered[h, e] = dot(picks, a_high[...]) + dot(picks, a_low[...])
            for n, partner in enumerate(partners):
                start(
                    ordered.at[h, e, pl.ds(pl.multiple_of(16 * partner, 16), 16)],
                    arrived.at[h, e, pl.ds(pl.multiple_of(16 * phi, 16), 16)],
                    s2.at[h, e, n],
                    r2.at[h, e, phi],
                    (theta, partner),
                )
            mine = pl.ds(pl.multiple_of(16 * phi, 16), 16)
            arrived[h, e, mine] = ordered[h, e, mine]

    for load in loads:
        load.wait()
    lax.fori_loop(0, 8, prepare, 0)
    for h in range(2):
        for partner in partners:
            spot = rows.at[h, partner]
            send(spot, spot, s1.at[h, 0], r1.at[h, partner], (theta, partner)).wait_recv()
        outer(h)
        inner()
        order_and_send(h)
        if h == 0:
            lax.fori_loop(8, 16, prepare, 0)

    wide = lax.broadcasted_iota(jnp.int32, (64, 128), 1)
    column = lax.broadcasted_iota(jnp.int32, (8, PAIR_LEN), 1)

    def arrive(e):
        for partner in partners:
            for h in range(2):
                spot = arrived.at[h, e, pl.ds(pl.multiple_of(16 * partner, 16), 16)]
                send(spot, spot, s2.at[h, e, 0], r2.at[h, e, partner], (theta, partner)).wait_recv()

        def body(slot, carry):
            turned = []
            for h in range(2):
                both = arrived[h, e, pl.ds(slot, 16, stride=16), :]
                both = jnp.concatenate([both[:8] + both[8:], both[:8] - both[8:]], axis=0)
                turned.append(
                    jnp.concatenate(
                        [
                            both if (32 * h - 32 * (2 * kind + p)) % 128 == 0
                            else pltpu.roll(both, (32 * h - 32 * (2 * kind + p)) % 128, 1)
                            for p in range(2) for kind in range(2)
                        ],
                        axis=0,
                    )
                )
            value = jnp.where(wide < 32, turned[0], turned[1])
            high = value.astype(BF16).astype(F32)
            low = pltpu.roll(value - high, 64, 1)
            left[slot, :, 0:128] = jnp.where(wide < 64, high, low).astype(BF16)
            left[slot, :, 128:256] = high.astype(BF16)
            return carry

        lax.fori_loop(0, 16, body, 0)

    def project(e, of_core):
        def body(n, carry):
            slot = 2 * n + of_core
            number = 2 * slot + e
            product = dot(left[slot, :, 0:192], weights[number])
            pair = pair_scalars[32 * phi + number]
            is_first = column < ORDERS - pair
            is_even = (column + jnp.where(is_first, 0, pair)) % 2 == 0
            for half in range(2):
                four = [product[32 * half + 8 * m : 32 * half + 8 * m + 8] for m in range(4)]
                lower = jnp.where(is_even, four[0], four[1])
                upper = jnp.where(is_even, four[2], four[3])
                part[e, of_core, n, 8 * half : 8 * half + 8, :] = jnp.where(is_first, lower, upper)
            return carry

        lax.fori_loop(0, 8, body, 0, unroll=2)

    y_up, y_down, y_far = (y + 1) % 4, (y + 3) % 4, (y + 2) % 4

    def to_core(e):
        project(e, 1 - core)
        copy = start(part.at[e, 1 - core], from_core.at[e], sa.at[e], ra.at[e], (core_mate, phi))
        project(e, core)
        return copy

    def to_ring(e, copy):
        copy.wait_recv()
        part[e, core] = part[e, core] + from_core[e]
        return [
            start(part.at[e, core, src], dst, sb.at[e, n], rb.at[e, n], (device, phi))
            for n, (src, dst, device) in enumerate((
                (2 * y_far, ring_in.at[e, 0], up),
                (2 * y_far + 1, ring_in.at[e, 1], down),
                (2 * y_up + 1, near_in.at[e, 0], up),
                (2 * y_down, near_in.at[e, 1], down),
            ))
        ]

    def join(e, near):
        copies = []
        for n, (src, device) in enumerate(((2 * y_up, up), (2 * y_down + 1, down))):
            near[n].wait_recv()
            joined[e, n] = part[e, core, src] + ring_in[e, n]
            copies.append(start(joined.at[e, n], joined_in.at[e, n], sc.at[e, n], rc.at[e, n], (device, phi)))
        return copies

    def to_far(e, near, last):
        for copy in near[2:] + last:
            copy.wait_recv()
        whole[e, 0] = part[e, core, 2 * y] + joined_in[e, 0] + near_in[e, 1]
        whole[e, 1] = part[e, core, 2 * y + 1] + joined_in[e, 1] + near_in[e, 0]
        return start(whole.at[e, 1 - far], from_far.at[e], sz.at[e], rz.at[e], (far_mate, phi))

    arrive(0)
    near0 = to_ring(0, to_core(0))
    arrive(1)
    core1 = to_core(1)
    last0 = join(0, near0)
    near1 = to_ring(1, core1)
    far0 = to_far(0, near0, last0)
    last1 = join(1, near1)
    far1 = to_far(1, near1, last1)
    for e, copy in enumerate((far0, far1)):
        copy.wait_recv()
        out[e] = whole[e, far] + from_far[e]

    for copy in sent:
        copy.wait_send()


def on_device(fields, legendre, pair_table):
    twiddle, inner_high, inner_low = dft_tables()
    vmem = pl.BlockSpec(memory_space=pltpu.VMEM)
    dma = pltpu.SemaphoreType.DMA
    row = (16, PAIR_LEN)
    result = pl.pallas_call(
        kernel,
        out_shape=jax.ShapeDtypeStruct((2, *row), F32),
        in_specs=[
            vmem,
            pl.BlockSpec(memory_space=pl.ANY),
            vmem,
            pl.BlockSpec(memory_space=pltpu.SMEM),
            vmem,
            vmem,
            vmem,
        ],
        out_specs=vmem,
        scratch_shapes=[
            pltpu.VMEM((64, 32, PAIR_LEN), F32),
            pltpu.VMEM((32, 192, PAIR_LEN), BF16),
            pltpu.VMEM((2, 16, 32, 256), F32),
            pltpu.VMEM((512, 512), BF16),
            pltpu.VMEM((512, 512), BF16),
            pltpu.VMEM((512, 128), BF16),
            pltpu.VMEM((512, 128), BF16),
            pltpu.VMEM((512, 128), F32),
            pltpu.VMEM((2, 256, 512), BF16),
            pltpu.VMEM((2, 2, 256, 128), F32),
            pltpu.VMEM((2, 2, 256, 128), F32),
            pltpu.VMEM((16, 64, 256), BF16),
            pltpu.VMEM((2, 2, 8, *row), F32),
            pltpu.VMEM((2, 8, *row), F32),
            pltpu.VMEM((2, 2, *row), F32),
            pltpu.VMEM((2, 2, *row), F32),
            pltpu.VMEM((2, 2, *row), F32),
            pltpu.VMEM((2, 2, *row), F32),
            pltpu.VMEM((2, 2, *row), F32),
            pltpu.VMEM((2, *row), F32),
            dma((4,)),
            dma((2, 15)), dma((2, 16)),
            dma((2, 2, 15)), dma((2, 2, 16)),
            dma((2,)), dma((2,)),
            dma((2, 4)), dma((2, 4)),
            dma((2, 2)), dma((2, 2)),
            dma((2,)), dma((2,)),
        ],
        compiler_params=pltpu.CompilerParams(
            collective_id=0, has_side_effects=True, vmem_limit_bytes=40 * 1024 * 1024
        ),
        name="harmonics",
    )(
        fields,
        legendre,
        pair_table.reshape(1, -1),
        pair_table,
        jnp.asarray(twiddle),
        jnp.asarray(inner_high),
        jnp.asarray(inner_low),
    )
    return result.reshape(2, 2, 8, PAIR_LEN)


def solution(mesh):
    placed = (P(None, None, "theta", "phi"), P("theta", "phi", None), P())
    return jax.shard_map(
        on_device,
        mesh=mesh,
        in_specs=placed,
        out_specs=P(("phi", "theta"), None, None, None),
        check_vma=False,
    )
```

```python
import functools
import math

import jax
import jax.numpy as jnp
import numpy as np
from jax import lax
from jax.experimental import pallas as pl
from jax.experimental.pallas import tpu as pltpu
from jax.sharding import PartitionSpec as P

LONS = 4096
ORDERS = 1024
PAIR_LEN = 1025

MESH = pl.DeviceIdType.MESH
F32 = jnp.float32
BF16 = jnp.bfloat16


def dft_tables():
    r = np.arange(16)
    k = np.arange(256)
    twiddle = 2.0 * np.pi * np.outer(r, k) / LONS
    a = np.arange(32)
    m1 = np.concatenate([64 + a, 127 - a])
    inner = 2.0 * np.pi * (np.outer(m1, k) % 256) / 256
    cos, sin = np.cos(inner), np.sin(inner)
    both = np.stack([np.concatenate([cos, sin], 1), np.concatenate([-sin, cos], 1)])
    both = both.reshape(2, 2, 32, 512).transpose(1, 0, 2, 3).reshape(128, 512)
    both = both.astype(np.float32)
    high = both.astype(BF16)
    low = (both - high.astype(np.float32)).astype(BF16)
    return np.stack([np.cos(twiddle), np.sin(twiddle)]).astype(np.float32), high, low


def halves(x):
    high = x.astype(BF16)
    return high, (x - high.astype(F32)).astype(BF16)


def weighted(terms):
    total = None
    for weight, value in terms:
        if abs(weight) < 1e-12:
            continue
        if abs(weight - 1.0) < 1e-12:
            total = value if total is None else total + value
        elif abs(weight + 1.0) < 1e-12:
            total = -value if total is None else total - value
        else:
            total = value * weight if total is None else total + value * weight
    return total


def sixteen_point(x):
    e = [None] + [x[j] + x[16 - j] for j in range(1, 8)]
    o = [None] + [x[j] - x[16 - j] for j in range(1, 8)]
    cos = lambda t: math.cos(math.pi * t / 8)
    sin = lambda t: math.sin(math.pi * t / 8)
    base = [x[0] + x[8], x[0] - x[8]]
    re_of, im_of = [], []
    plus_e = [e[j] + e[8 - j] for j in range(1, 4)]
    less_e = [e[j] - e[8 - j] for j in range(1, 4)]
    plus_o = [o[j] + o[8 - j] for j in range(1, 4)]
    less_o = [o[j] - o[8 - j] for j in range(1, 4)]
    for r in range(9):
        fold_e, fold_o = (less_e, plus_o) if r % 2 else (plus_e, less_o)
        re_terms = [(1.0, base[r % 2])] + [(cos(j * r), fold_e[j - 1]) for j in (1, 2, 3)]
        im_terms = [(-sin(j * r), fold_o[j - 1]) for j in (1, 2, 3)]
        if r % 2:
            im_terms.append((-sin(4 * r), o[4]))
        else:
            re_terms.append((cos(4 * r), e[4]))
        re_of.append(weighted(re_terms))
        im_of.append(weighted(im_terms))
    return re_of, im_of


def dot(a, b):
    return lax.dot_general(a, b, (((1,), (0,)), ((), ())), preferred_element_type=F32)


def dot_rows(a, b):
    return lax.dot_general(a, b, (((1,), (1,)), ((), ())), preferred_element_type=F32)


def kernel(
    fields_in, legendre, pairs_in, pair_scalars, twiddle_in, high_in, low_in, out,
    fields, pairs, twiddle, inner_high, inner_low,
    staged, weights, rows, z_high, z_low, a_high, a_low, spread_pairs, chosen, ordered, arrived,
    left, part, from_core, ring_in, near_in, joined, joined_in, whole, from_far,
    leg_sem, in_sem, s1, r1, s2, r2, sa, ra, sb, rb, sc, rc, sz, rz,
):
    theta = lax.axis_index("theta")
    phi = lax.axis_index("phi")
    z, x = phi // 4, phi % 4
    y, far, core = theta // 4, (theta // 2) % 2, theta % 2
    core_mate = theta + 1 - 2 * core
    far_mate = theta + 2 - 4 * far
    up = ((y + 1) % 4) * 4 + theta % 4
    down = ((y + 3) % 4) * 4 + theta % 4

    inputs = [
        pltpu.make_async_copy(src, dst, in_sem.at[n])
        for n, (src, dst) in enumerate((
            (fields_in, fields),
            (pairs_in, pairs),
            (twiddle_in, twiddle),
            (high_in, inner_high),
            (low_in, inner_low),
        ))
    ]
    for load in inputs:
        load.start()
    loads = [
        pltpu.make_async_copy(legendre.at[pl.ds(16 * c, 16)], staged.at[pl.ds(16 * c, 16)], leg_sem.at[c])
        for c in range(4)
    ]
    for load in loads:
        load.start()

    z_order = [(z + 2) % 4, 3 - z, z + 1 - 2 * (z % 2), z]
    partners = []
    for step, other_z in enumerate(z_order):
        for dx in range(4):
            if step == 3 and dx == 0:
                continue
            partners.append(other_z * 4 + (x + dx) % 4)

    barrier = pltpu.get_barrier_semaphore()
    for partner in partners:
        pl.semaphore_signal(barrier, inc=1, device_id=(theta, partner), device_id_type=MESH)
    for partner in (core_mate, far_mate, up, down):
        pl.semaphore_signal(barrier, inc=1, device_id=(partner, phi), device_id_type=MESH)
    pl.semaphore_wait(barrier, 19)
    inputs[0].wait()

    def send(src, dst, send_sem, recv_sem, device):
        return pltpu.make_async_remote_copy(
            src_ref=src, dst_ref=dst, send_sem=send_sem, recv_sem=recv_sem, device_id=device, device_id_type=MESH
        )

    sent = []

    def start(*copy_args):
        copy = send(*copy_args)
        copy.start()
        sent.append(copy)
        return copy

    for h in range(2):
        lats = pl.ds(32 * h, 32)
        for n, partner in enumerate(partners):
            start(
                fields.at[partner % 8, partner // 8, lats],
                rows.at[h, phi],
                s1.at[h, n],
                r1.at[h, phi],
                (theta, partner),
            )
        rows[h, phi] = fields[phi % 8, phi // 8, lats]

    for load in inputs[1:]:
        load.wait()

    spread = jnp.broadcast_to(pairs[...].astype(F32), (128, 512))
    for block in range(4):
        at = slice(128 * block, 128 * block + 128)
        spread_pairs[at, :] = jnp.transpose(spread[:, at])
    lane = lax.broadcasted_iota(jnp.int32, (128, 128), 1)
    upper_half = lax.broadcasted_iota(jnp.int32, (16, 8, 128), 1) >= 4
    for block in range(2):
        own = spread_pairs[256 * block : 256 * block + 256, :].reshape(16, 16, 128)
        one, two = own[:, :8], own[:, 8:]
        low = jnp.where(upper_half, pltpu.roll(two, 4, 1), one).reshape(128, 128)
        top = jnp.where(upper_half, two, pltpu.roll(one, 4, 1)).reshape(128, 128)
        for turn, picked in enumerate((jnp.where(far == 0, top, low), jnp.where(far == 0, low, top))):
            for tile in range(4):
                code = (16 * (lane % 32) + (4 * tile + lane // 32)).astype(F32)
                chosen[turn, 128 * block : 128 * block + 128, 128 * tile : 128 * tile + 128] = jnp.where(
                    picked == code, 1.0, 0.0
                ).astype(BF16)

    def prepare(n, carry):
        lat, slot = 16 * (n // 4), 8 * (n % 4)
        for tile in range(9):
            lanes = slice(128 * tile, min(128 * tile + 128, PAIR_LEN))
            block = staged[pl.ds(lat, 16), pl.ds(slot, 8), lanes]
            high, low = halves(jnp.transpose(block, (1, 0, 2)))
            weights[pl.ds(slot, 8), pl.ds(lat, 16), lanes] = high
            weights[pl.ds(slot, 8), pl.ds(64 + lat, 16), lanes] = high
            weights[pl.ds(slot, 8), pl.ds(128 + lat, 16), lanes] = low
        return carry

    def outer(h):
        def body(n, carry):
            lat = pl.multiple_of(16 * (n // 2), 16)
            lanes = pl.ds(pl.multiple_of(128 * (n % 2), 128), 128)
            upper = pl.ds(pl.multiple_of(256 + 128 * (n % 2), 128), 128)
            re_of, im_of = sixteen_point([rows[h, p, pl.ds(lat, 16), lanes] for p in range(16)])
            for r in range(16):
                re = re_of[min(r, 16 - r)]
                im = im_of[min(r, 16 - r)]
                c = twiddle[0, r : r + 1, lanes]
                s = twiddle[1, r : r + 1, lanes]
                if im is None:
                    z_re, z_im = re * c, -(re * s)
                elif r <= 8:
                    z_re, z_im = re * c + im * s, im * c - re * s
                else:
                    z_re, z_im = re * c - im * s, -(im * c + re * s)
                for value, at in ((z_re, lanes), (z_im, upper)):
                    high, low = halves(value)
                    z_high[pl.ds(32 * r + lat, 16), at] = high
                    z_low[pl.ds(32 * r + lat, 16), at] = low
            return carry

        lax.fori_loop(0, 4, body, 0)

    def inner():
        for group in range(4):
            at = slice(128 * group, 128 * group + 128)
            high, low = z_high[at, :], z_low[at, :]
            both = dot_rows(inner_high[...], high) + dot_rows(inner_high[...], low) + dot_rows(inner_low[...], high)
            for j in range(4):
                lats = slice(32 * j, 32 * j + 32)
                r = 4 * group + j
                for kind, spot in ((0, r), (1, 15 - r)):
                    value = jnp.concatenate(
                        [both[64 * kind : 64 * kind + 32, lats], both[64 * kind + 32 : 64 * kind + 64, lats]], axis=1
                    )
                    high_value, low_value = halves(value)
                    a_high[32 * spot : 32 * spot + 32, 64 * kind : 64 * kind + 64] = high_value
                    a_low[32 * spot : 32 * spot + 32, 64 * kind : 64 * kind + 64] = low_value

    def put_in_order(h):
        for turn in range(2):
            picks = chosen[turn]
            ordered[h, turn] = dot(picks, a_high[...]) + dot(picks, a_low[...])

    def send_orders(h):
        for turn in range(2):
            for n, partner in enumerate(partners):
                start(
                    ordered.at[h, turn, pl.ds(pl.multiple_of(16 * partner, 16), 16)],
                    arrived.at[h, turn, pl.ds(pl.multiple_of(16 * phi, 16), 16)],
                    s2.at[h, turn, n],
                    r2.at[h, turn, phi],
                    (theta, partner),
                )
            mine = pl.ds(pl.multiple_of(16 * phi, 16), 16)
            arrived[h, turn, mine] = ordered[h, turn, mine]

    def receive_rows(h):
        for partner in partners:
            spot = rows.at[h, partner]
            send(spot, spot, s1.at[h, 0], r1.at[h, partner], (theta, partner)).wait_recv()

    for load in loads:
        load.wait()
    lax.fori_loop(0, 8, prepare, 0)
    receive_rows(0)
    outer(0)
    inner()
    put_in_order(0)
    lax.fori_loop(8, 16, prepare, 0)
    receive_rows(1)
    send_orders(0)
    outer(1)
    inner()
    put_in_order(1)
    send_orders(1)

    wide = lax.broadcasted_iota(jnp.int32, (64, 128), 1)
    column = lax.broadcasted_iota(jnp.int32, (8, PAIR_LEN), 1)

    def arrive(turn):
        for partner in partners:
            for h in range(2):
                spot = arrived.at[h, turn, pl.ds(pl.multiple_of(16 * partner, 16), 16)]
                send(spot, spot, s2.at[h, turn, 0], r2.at[h, turn, partner], (theta, partner)).wait_recv()

        def body(slot, carry):
            turned = []
            for h in range(2):
                both = arrived[h, turn, pl.ds(slot, 16, stride=16), :]
                both = jnp.concatenate([both[:8] + both[8:], both[:8] - both[8:]], axis=0)
                turned.append(
                    jnp.concatenate(
                        [
                            both if (32 * h - 32 * (2 * kind + p)) % 128 == 0
                            else pltpu.roll(both, (32 * h - 32 * (2 * kind + p)) % 128, 1)
                            for p in range(2) for kind in range(2)
                        ],
                        axis=0,
                    )
                )
            value = jnp.where(wide < 32, turned[0], turned[1])
            high = value.astype(BF16).astype(F32)
            low = pltpu.roll(value - high, 64, 1)
            left[slot, :, 0:128] = jnp.where(wide < 64, high, low).astype(BF16)
            left[slot, :, 128:256] = high.astype(BF16)
            return carry

        lax.fori_loop(0, 16, body, 0, unroll=4)

    def project(turn, e, of_core):
        z_half = far if turn else 1 - far

        def body(n, carry):
            number = 8 * n + 4 * z_half + 2 * of_core + e
            product = dot(left[4 * n + 2 * of_core + e, :, 0:192], weights[number])
            pair = pair_scalars[32 * phi + number]
            is_first = column < ORDERS - pair
            is_even = (column + jnp.where(is_first, 0, pair)) % 2 == 0
            for half in range(2):
                four = [product[32 * half + 8 * m : 32 * half + 8 * m + 8] for m in range(4)]
                lower = jnp.where(is_even, four[0], four[1])
                upper = jnp.where(is_even, four[2], four[3])
                part[turn, e, of_core, n, half] = jnp.where(is_first, lower, upper)
            return carry

        lax.fori_loop(0, 4, body, 0, unroll=4)

    y_up, y_down, y_far = (y + 1) % 4, (y + 3) % 4, (y + 2) % 4

    def to_core(turn, e):
        project(turn, e, 1 - core)
        copy = start(
            part.at[turn, e, 1 - core], from_core.at[turn, e], sa.at[turn, e], ra.at[turn, e], (core_mate, phi)
        )
        project(turn, e, core)
        return copy

    def to_ring(turn, e, copy):
        copy.wait_recv()
        part[turn, e, core] = part[turn, e, core] + from_core[turn, e]
        return [
            start(
                part.at[turn, e, core, to_y, half], dst, sb.at[turn, e, n], rb.at[turn, e, n], (device, phi)
            )
            for n, (to_y, half, dst, device) in enumerate((
                (y_far, 0, ring_in.at[turn, e, 0], up),
                (y_far, 1, ring_in.at[turn, e, 1], down),
                (y_up, 1, near_in.at[turn, e, 0], up),
                (y_down, 0, near_in.at[turn, e, 1], down),
            ))
        ]

    def join(turn, e, near):
        copies = []
        for n, (to_y, device) in enumerate(((y_up, up), (y_down, down))):
            near[n].wait_recv()
            joined[turn, e, n] = part[turn, e, core, to_y, n] + ring_in[turn, e, n]
            copies.append(
                start(
                    joined.at[turn, e, n],
                    joined_in.at[turn, e, n],
                    sc.at[turn, e, n],
                    rc.at[turn, e, n],
                    (device, phi),
                )
            )
        return copies

    def finish(turn, e, near, last):
        for copy in near[2:] + last:
            copy.wait_recv()
        for half in range(2):
            whole[turn, e, half] = (
                part[turn, e, core, y, half] + joined_in[turn, e, half] + near_in[turn, e, 1 - half]
            )
        if turn == 0:
            return start(whole.at[0, e], from_far.at[e], sz.at[e], rz.at[e], (far_mate, phi))

    arrive(0)
    core00 = to_core(0, 0)
    core01 = to_core(0, 1)
    near00 = to_ring(0, 0, core00)
    arrive(1)
    near01 = to_ring(0, 1, core01)
    core10 = to_core(1, 0)
    last00 = join(0, 0, near00)
    core11 = to_core(1, 1)
    near10 = to_ring(1, 0, core10)
    last01 = join(0, 1, near01)
    far0 = finish(0, 0, near00, last00)
    near11 = to_ring(1, 1, core11)
    far1 = finish(0, 1, near01, last01)
    last10 = join(1, 0, near10)
    last11 = join(1, 1, near11)
    finish(1, 0, near10, last10)
    finish(1, 1, near11, last11)
    for e, copy in enumerate((far0, far1)):
        copy.wait_recv()
        out[e] = whole[1, e] + from_far[e]

    for copy in sent:
        copy.wait_send()


def on_device(fields, legendre, pair_table):
    twiddle, inner_high, inner_low = dft_tables()
    vmem = pl.BlockSpec(memory_space=pltpu.VMEM)
    anywhere = pl.BlockSpec(memory_space=pl.ANY)
    dma = pltpu.SemaphoreType.DMA
    row = (2, 8, PAIR_LEN)
    result = pl.pallas_call(
        kernel,
        out_shape=jax.ShapeDtypeStruct((2, *row), F32),
        in_specs=[
            anywhere,
            anywhere,
            anywhere,
            pl.BlockSpec(memory_space=pltpu.SMEM),
            anywhere,
            anywhere,
            anywhere,
        ],
        out_specs=vmem,
        scratch_shapes=[
            pltpu.VMEM(fields.shape, F32),
            pltpu.VMEM((1, 512), jnp.int32),
            pltpu.VMEM((2, 16, 256), F32),
            pltpu.VMEM((128, 512), BF16),
            pltpu.VMEM((128, 512), BF16),
            pltpu.VMEM((64, 32, PAIR_LEN), F32),
            pltpu.VMEM((32, 192, PAIR_LEN), BF16),
            pltpu.VMEM((2, 16, 32, 256), F32),
            pltpu.VMEM((512, 512), BF16),
            pltpu.VMEM((512, 512), BF16),
            pltpu.VMEM((512, 128), BF16),
            pltpu.VMEM((512, 128), BF16),
            pltpu.VMEM((512, 128), F32),
            pltpu.VMEM((2, 256, 512), BF16),
            pltpu.VMEM((2, 2, 256, 128), F32),
            pltpu.VMEM((2, 2, 256, 128), F32),
            pltpu.VMEM((16, 64, 256), BF16),
            pltpu.VMEM((2, 2, 2, 4, *row), F32),
            pltpu.VMEM((2, 2, 4, *row), F32),
            pltpu.VMEM((2, 2, *row), F32),
            pltpu.VMEM((2, 2, *row), F32),
            pltpu.VMEM((2, 2, *row), F32),
            pltpu.VMEM((2, 2, *row), F32),
            pltpu.VMEM((2, 2, *row), F32),
            pltpu.VMEM((2, *row), F32),
            dma((4,)),
            dma((5,)),
            dma((2, 15)), dma((2, 16)),
            dma((2, 2, 15)), dma((2, 2, 16)),
            dma((2, 2)), dma((2, 2)),
            dma((2, 2, 4)), dma((2, 2, 4)),
            dma((2, 2, 2)), dma((2, 2, 2)),
            dma((2,)), dma((2,)),
        ],
        compiler_params=pltpu.CompilerParams(
            collective_id=0, has_side_effects=True, vmem_limit_bytes=60000 * 1024
        ),
        name="harmonics",
    )(
        fields,
        legendre,
        pair_table.reshape(1, -1),
        pair_table,
        jnp.asarray(twiddle),
        jnp.asarray(inner_high),
        jnp.asarray(inner_low),
    )
    return result


def solution(mesh):
    placed = (P(None, None, "theta", "phi"), P("theta", "phi", None), P())
    return jax.shard_map(
        on_device,
        mesh=mesh,
        in_specs=placed,
        out_specs=P(("phi", "theta"), None, None, None),
        check_vma=False,
    )
```

```python
import functools
import math

import jax
import jax.numpy as jnp
import numpy as np
from jax import lax
from jax.experimental import pallas as pl
from jax.experimental.pallas import tpu as pltpu
from jax.sharding import PartitionSpec as P

LONS = 4096
ORDERS = 1024
PAIR_LEN = 1025

MESH = pl.DeviceIdType.MESH
F32 = jnp.float32
BF16 = jnp.bfloat16


def dft_tables():
    r = np.arange(16)
    k = np.arange(256)
    twiddle = 2.0 * np.pi * np.outer(r, k) / LONS
    a = np.arange(32)
    m1 = np.concatenate([64 + a, 127 - a])
    inner = 2.0 * np.pi * (np.outer(m1, k) % 256) / 256
    cos, sin = np.cos(inner), np.sin(inner)
    both = np.stack([np.concatenate([cos, sin], 1), np.concatenate([-sin, cos], 1)])
    both = both.reshape(2, 2, 32, 512).transpose(1, 0, 2, 3).reshape(128, 512)
    both = both.astype(np.float32)
    high = both.astype(BF16)
    low = (both - high.astype(np.float32)).astype(BF16)
    return np.stack([np.cos(twiddle), np.sin(twiddle)]).astype(np.float32), high, low


def halves(x):
    high = x.astype(BF16)
    return high, (x - high.astype(F32)).astype(BF16)


def weighted(terms):
    total = None
    for weight, value in terms:
        if abs(weight) < 1e-12:
            continue
        if abs(weight - 1.0) < 1e-12:
            total = value if total is None else total + value
        elif abs(weight + 1.0) < 1e-12:
            total = -value if total is None else total - value
        else:
            total = value * weight if total is None else total + value * weight
    return total


def sixteen_point(x):
    e = [None] + [x[j] + x[16 - j] for j in range(1, 8)]
    o = [None] + [x[j] - x[16 - j] for j in range(1, 8)]
    cos = lambda t: math.cos(math.pi * t / 8)
    sin = lambda t: math.sin(math.pi * t / 8)
    base = [x[0] + x[8], x[0] - x[8]]
    re_of, im_of = [], []
    plus_e = [e[j] + e[8 - j] for j in range(1, 4)]
    less_e = [e[j] - e[8 - j] for j in range(1, 4)]
    plus_o = [o[j] + o[8 - j] for j in range(1, 4)]
    less_o = [o[j] - o[8 - j] for j in range(1, 4)]
    for r in range(9):
        fold_e, fold_o = (less_e, plus_o) if r % 2 else (plus_e, less_o)
        re_terms = [(1.0, base[r % 2])] + [(cos(j * r), fold_e[j - 1]) for j in (1, 2, 3)]
        im_terms = [(-sin(j * r), fold_o[j - 1]) for j in (1, 2, 3)]
        if r % 2:
            im_terms.append((-sin(4 * r), o[4]))
        else:
            re_terms.append((cos(4 * r), e[4]))
        re_of.append(weighted(re_terms))
        im_of.append(weighted(im_terms))
    return re_of, im_of


def dot(a, b):
    return lax.dot_general(a, b, (((1,), (0,)), ((), ())), preferred_element_type=F32)


def dot_rows(a, b):
    return lax.dot_general(a, b, (((1,), (1,)), ((), ())), preferred_element_type=F32)


def kernel(
    fields_in, legendre, pairs_in, pair_scalars, twiddle_in, high_in, low_in, out,
    fields, pairs, twiddle, inner_high, inner_low,
    staged, weights, rows, z_high, z_low, a_high, a_low, spread_pairs, chosen, ordered, arrived,
    left, part, from_core, ring_in, near_in, joined, joined_in, whole, from_far,
    leg_sem, in_sem, s1, r1, s2, r2, sa, ra, sb, rb, sc, rc, sz, rz,
):
    theta = lax.axis_index("theta")
    phi = lax.axis_index("phi")
    z, x = phi // 4, phi % 4
    y, far, core = theta // 4, (theta // 2) % 2, theta % 2
    core_mate = theta + 1 - 2 * core
    far_mate = theta + 2 - 4 * far
    up = ((y + 1) % 4) * 4 + theta % 4
    down = ((y + 3) % 4) * 4 + theta % 4

    inputs = [
        pltpu.make_async_copy(src, dst, in_sem.at[n])
        for n, (src, dst) in enumerate((
            (fields_in, fields),
            (pairs_in, pairs),
            (twiddle_in, twiddle),
            (high_in, inner_high),
            (low_in, inner_low),
        ))
    ]
    for load in inputs:
        load.start()
    loads = [
        pltpu.make_async_copy(legendre.at[pl.ds(16 * c, 16)], staged.at[pl.ds(16 * c, 16)], leg_sem.at[c])
        for c in range(4)
    ]
    for load in loads:
        load.start()

    z_order = [(z + 2) % 4, 3 - z, z + 1 - 2 * (z % 2), z]
    partners = []
    for step, other_z in enumerate(z_order):
        for dx in range(4):
            if step == 3 and dx == 0:
                continue
            partners.append(other_z * 4 + (x + dx) % 4)

    barrier = pltpu.get_barrier_semaphore()
    for partner in partners:
        pl.semaphore_signal(barrier, inc=1, device_id=(theta, partner), device_id_type=MESH)
    for partner in (core_mate, far_mate, up, down):
        pl.semaphore_signal(barrier, inc=1, device_id=(partner, phi), device_id_type=MESH)
    pl.semaphore_wait(barrier, 19)
    inputs[0].wait()

    def send(src, dst, send_sem, recv_sem, device):
        return pltpu.make_async_remote_copy(
            src_ref=src, dst_ref=dst, send_sem=send_sem, recv_sem=recv_sem, device_id=device, device_id_type=MESH
        )

    sent = []

    def start(*copy_args):
        copy = send(*copy_args)
        copy.start()
        sent.append(copy)
        return copy

    for h in range(2):
        lats = pl.ds(32 * h, 32)
        for n, partner in enumerate(partners):
            start(
                fields.at[partner % 8, partner // 8, lats],
                rows.at[h, phi],
                s1.at[h, n],
                r1.at[h, phi],
                (theta, partner),
            )
        rows[h, phi] = fields[phi % 8, phi // 8, lats]

    for load in inputs[1:]:
        load.wait()

    spread = jnp.broadcast_to(pairs[...].astype(F32), (128, 512))
    for block in range(4):
        at = slice(128 * block, 128 * block + 128)
        spread_pairs[at, :] = jnp.transpose(spread[:, at])
    lane = lax.broadcasted_iota(jnp.int32, (128, 128), 1)
    upper_half = lax.broadcasted_iota(jnp.int32, (16, 8, 128), 1) >= 4
    for block in range(2):
        own = spread_pairs[256 * block : 256 * block + 256, :].reshape(16, 16, 128)
        one, two = own[:, :8], own[:, 8:]
        low = jnp.where(upper_half, pltpu.roll(two, 4, 1), one).reshape(128, 128)
        top = jnp.where(upper_half, two, pltpu.roll(one, 4, 1)).reshape(128, 128)
        for turn, picked in enumerate((jnp.where(far == 0, top, low), jnp.where(far == 0, low, top))):
            for tile in range(4):
                code = (16 * (lane % 32) + (4 * tile + lane // 32)).astype(F32)
                chosen[turn, 128 * block : 128 * block + 128, 128 * tile : 128 * tile + 128] = jnp.where(
                    picked == code, 1.0, 0.0
                ).astype(BF16)

    def prepare(n, carry):
        lat, slot = 16 * (n // 4), 8 * (n % 4)
        for tile in range(9):
            lanes = slice(128 * tile, min(128 * tile + 128, PAIR_LEN))
            block = staged[pl.ds(lat, 16), pl.ds(slot, 8), lanes]
            high, low = halves(jnp.transpose(block, (1, 0, 2)))
            weights[pl.ds(slot, 8), pl.ds(lat, 16), lanes] = high
            weights[pl.ds(slot, 8), pl.ds(64 + lat, 16), lanes] = high
            weights[pl.ds(slot, 8), pl.ds(128 + lat, 16), lanes] = low
        return carry

    def outer(h):
        def body(n, carry):
            lat = pl.multiple_of(16 * (n // 2), 16)
            lanes = pl.ds(pl.multiple_of(128 * (n % 2), 128), 128)
            upper = pl.ds(pl.multiple_of(256 + 128 * (n % 2), 128), 128)
            re_of, im_of = sixteen_point([rows[h, p, pl.ds(lat, 16), lanes] for p in range(16)])
            for r in range(16):
                re = re_of[min(r, 16 - r)]
                im = im_of[min(r, 16 - r)]
                c = twiddle[0, r : r + 1, lanes]
                s = twiddle[1, r : r + 1, lanes]
                if im is None:
                    z_re, z_im = re * c, -(re * s)
                elif r <= 8:
                    z_re, z_im = re * c + im * s, im * c - re * s
                else:
                    z_re, z_im = re * c - im * s, -(im * c + re * s)
                for value, at in ((z_re, lanes), (z_im, upper)):
                    high, low = halves(value)
                    z_high[pl.ds(32 * r + lat, 16), at] = high
                    z_low[pl.ds(32 * r + lat, 16), at] = low
            return carry

        lax.fori_loop(0, 4, body, 0)

    def inner():
        for group in range(4):
            at = slice(128 * group, 128 * group + 128)
            high, low = z_high[at, :], z_low[at, :]
            both = dot_rows(inner_high[...], high) + dot_rows(inner_high[...], low) + dot_rows(inner_low[...], high)
            for j in range(4):
                lats = slice(32 * j, 32 * j + 32)
                r = 4 * group + j
                for kind, spot in ((0, r), (1, 15 - r)):
                    value = jnp.concatenate(
                        [both[64 * kind : 64 * kind + 32, lats], both[64 * kind + 32 : 64 * kind + 64, lats]], axis=1
                    )
                    high_value, low_value = halves(value)
                    a_high[32 * spot : 32 * spot + 32, 64 * kind : 64 * kind + 64] = high_value
                    a_low[32 * spot : 32 * spot + 32, 64 * kind : 64 * kind + 64] = low_value

    def put_in_order(h):
        for turn in range(2):
            picks = chosen[turn]
            ordered[h, turn] = dot(picks, a_high[...]) + dot(picks, a_low[...])

    def send_orders(h, turn):
        for n, partner in enumerate(partners):
            start(
                ordered.at[h, turn, pl.ds(pl.multiple_of(16 * partner, 16), 16)],
                arrived.at[h, turn, pl.ds(pl.multiple_of(16 * phi, 16), 16)],
                s2.at[h, turn, n],
                r2.at[h, turn, phi],
                (theta, partner),
            )
        mine = pl.ds(pl.multiple_of(16 * phi, 16), 16)
        arrived[h, turn, mine] = ordered[h, turn, mine]

    def receive_rows(h):
        for partner in partners:
            spot = rows.at[h, partner]
            send(spot, spot, s1.at[h, 0], r1.at[h, partner], (theta, partner)).wait_recv()

    for load in loads:
        load.wait()
    lax.fori_loop(0, 8, prepare, 0)
    receive_rows(0)
    outer(0)
    inner()
    put_in_order(0)
    lax.fori_loop(8, 16, prepare, 0)
    receive_rows(1)
    send_orders(0, 0)
    outer(1)
    inner()
    put_in_order(1)
    send_orders(1, 0)
    send_orders(0, 1)
    send_orders(1, 1)

    wide = lax.broadcasted_iota(jnp.int32, (64, 128), 1)
    column = lax.broadcasted_iota(jnp.int32, (8, PAIR_LEN), 1)

    def arrive(turn):
        for partner in partners:
            for h in range(2):
                spot = arrived.at[h, turn, pl.ds(pl.multiple_of(16 * partner, 16), 16)]
                send(spot, spot, s2.at[h, turn, 0], r2.at[h, turn, partner], (theta, partner)).wait_recv()

        def body(slot, carry):
            turned = []
            for h in range(2):
                both = arrived[h, turn, pl.ds(slot, 16, stride=16), :]
                both = jnp.concatenate([both[:8] + both[8:], both[:8] - both[8:]], axis=0)
                turned.append(
                    jnp.concatenate(
                        [
                            both if (32 * h - 32 * (2 * kind + p)) % 128 == 0
                            else pltpu.roll(both, (32 * h - 32 * (2 * kind + p)) % 128, 1)
                            for p in range(2) for kind in range(2)
                        ],
                        axis=0,
                    )
                )
            value = jnp.where(wide < 32, turned[0], turned[1])
            high = value.astype(BF16).astype(F32)
            low = pltpu.roll(value - high, 64, 1)
            left[slot, :, 0:128] = jnp.where(wide < 64, high, low).astype(BF16)
            left[slot, :, 128:256] = high.astype(BF16)
            return carry

        lax.fori_loop(0, 16, body, 0, unroll=4)

    def project(turn, e, of_core):
        z_half = far if turn else 1 - far

        def body(n, carry):
            number = 8 * n + 4 * z_half + 2 * of_core + e
            product = dot(left[4 * n + 2 * of_core + e, :, 0:192], weights[number])
            pair = pair_scalars[32 * phi + number]
            is_first = column < ORDERS - pair
            is_even = (column + jnp.where(is_first, 0, pair)) % 2 == 0
            for half in range(2):
                four = [product[32 * half + 8 * m : 32 * half + 8 * m + 8] for m in range(4)]
                lower = jnp.where(is_even, four[0], four[1])
                upper = jnp.where(is_even, four[2], four[3])
                part[turn, e, of_core, n, half] = jnp.where(is_first, lower, upper)
            return carry

        lax.fori_loop(0, 4, body, 0, unroll=4)

    y_up, y_down, y_far = (y + 1) % 4, (y + 3) % 4, (y + 2) % 4

    def to_core(turn, e):
        project(turn, e, 1 - core)
        copy = start(
            part.at[turn, e, 1 - core], from_core.at[turn, e], sa.at[turn, e], ra.at[turn, e], (core_mate, phi)
        )
        project(turn, e, core)
        return copy

    def to_ring(turn, e, copy):
        copy.wait_recv()
        part[turn, e, core] = part[turn, e, core] + from_core[turn, e]
        return [
            start(
                part.at[turn, e, core, to_y, half], dst, sb.at[turn, e, n], rb.at[turn, e, n], (device, phi)
            )
            for n, (to_y, half, dst, device) in enumerate((
                (y_far, 0, ring_in.at[turn, e, 0], up),
                (y_far, 1, ring_in.at[turn, e, 1], down),
                (y_up, 1, near_in.at[turn, e, 0], up),
                (y_down, 0, near_in.at[turn, e, 1], down),
            ))
        ]

    def join(turn, e, near):
        copies = []
        for n, (to_y, device) in enumerate(((y_up, up), (y_down, down))):
            near[n].wait_recv()
            joined[turn, e, n] = part[turn, e, core, to_y, n] + ring_in[turn, e, n]
            copies.append(
                start(
                    joined.at[turn, e, n],
                    joined_in.at[turn, e, n],
                    sc.at[turn, e, n],
                    rc.at[turn, e, n],
                    (device, phi),
                )
            )
        return copies

    def finish(turn, e, near, last):
        for copy in near[2:] + last:
            copy.wait_recv()
        for half in range(2):
            whole[turn, e, half] = (
                part[turn, e, core, y, half] + joined_in[turn, e, half] + near_in[turn, e, 1 - half]
            )
        if turn == 0:
            return start(whole.at[0, e], from_far.at[e], sz.at[e], rz.at[e], (far_mate, phi))

    arrive(0)
    core00 = to_core(0, 0)
    near00 = to_ring(0, 0, core00)
    core01 = to_core(0, 1)
    near01 = to_ring(0, 1, core01)
    arrive(1)
    core10 = to_core(1, 0)
    last00 = join(0, 0, near00)
    core11 = to_core(1, 1)
    last01 = join(0, 1, near01)
    near10 = to_ring(1, 0, core10)
    far0 = finish(0, 0, near00, last00)
    near11 = to_ring(1, 1, core11)
    far1 = finish(0, 1, near01, last01)
    last10 = join(1, 0, near10)
    last11 = join(1, 1, near11)
    finish(1, 0, near10, last10)
    finish(1, 1, near11, last11)
    for e, copy in enumerate((far0, far1)):
        copy.wait_recv()
        out[e] = whole[1, e] + from_far[e]

    for copy in sent:
        copy.wait_send()


def on_device(fields, legendre, pair_table):
    twiddle, inner_high, inner_low = dft_tables()
    vmem = pl.BlockSpec(memory_space=pltpu.VMEM)
    anywhere = pl.BlockSpec(memory_space=pltpu.HBM)
    dma = pltpu.SemaphoreType.DMA
    row = (2, 8, PAIR_LEN)
    result = pl.pallas_call(
        kernel,
        out_shape=pltpu.VMEM((2, *row), F32),
        in_specs=[
            anywhere,
            anywhere,
            anywhere,
            pl.BlockSpec(memory_space=pltpu.SMEM),
            anywhere,
            anywhere,
            anywhere,
        ],
        out_specs=vmem,
        scratch_shapes=[
            pltpu.VMEM(fields.shape, F32),
            pltpu.VMEM((1, 512), jnp.int32),
            pltpu.VMEM((2, 16, 256), F32),
            pltpu.VMEM((128, 512), BF16),
            pltpu.VMEM((128, 512), BF16),
            pltpu.VMEM((64, 32, PAIR_LEN), F32),
            pltpu.VMEM((32, 192, PAIR_LEN), BF16),
            pltpu.VMEM((2, 16, 32, 256), F32),
            pltpu.VMEM((512, 512), BF16),
            pltpu.VMEM((512, 512), BF16),
            pltpu.VMEM((512, 128), BF16),
            pltpu.VMEM((512, 128), BF16),
            pltpu.VMEM((512, 128), F32),
            pltpu.VMEM((2, 256, 512), BF16),
            pltpu.VMEM((2, 2, 256, 128), F32),
            pltpu.VMEM((2, 2, 256, 128), F32),
            pltpu.VMEM((16, 64, 256), BF16),
            pltpu.VMEM((2, 2, 2, 4, *row), F32),
            pltpu.VMEM((2, 2, 4, *row), F32),
            pltpu.VMEM((2, 2, *row), F32),
            pltpu.VMEM((2, 2, *row), F32),
            pltpu.VMEM((2, 2, *row), F32),
            pltpu.VMEM((2, 2, *row), F32),
            pltpu.VMEM((2, 2, *row), F32),
            pltpu.VMEM((2, *row), F32),
            dma((4,)),
            dma((5,)),
            dma((2, 15)), dma((2, 16)),
            dma((2, 2, 15)), dma((2, 2, 16)),
            dma((2, 2)), dma((2, 2)),
            dma((2, 2, 4)), dma((2, 2, 4)),
            dma((2, 2, 2)), dma((2, 2, 2)),
            dma((2,)), dma((2,)),
        ],
        compiler_params=pltpu.CompilerParams(
            collective_id=0, has_side_effects=True, vmem_limit_bytes=60000 * 1024
        ),
        name="harmonics",
    )(
        fields,
        legendre,
        pair_table.reshape(1, -1),
        pair_table,
        jnp.asarray(twiddle),
        jnp.asarray(inner_high),
        jnp.asarray(inner_low),
    )
    return result


def solution(mesh):
    placed = (P(None, None, "theta", "phi"), P("theta", "phi", None), P())
    return jax.shard_map(
        on_device,
        mesh=mesh,
        in_specs=placed,
        out_specs=P(("phi", "theta"), None, None, None),
        check_vma=False,
    )
```

```python
import functools
import math

import jax
import jax.numpy as jnp
import numpy as np
from jax import lax
from jax.experimental import pallas as pl
from jax.experimental.pallas import tpu as pltpu
from jax.sharding import PartitionSpec as P

LONS = 4096
ORDERS = 1024
PAIR_LEN = 1025

MESH = pl.DeviceIdType.MESH
F32 = jnp.float32
BF16 = jnp.bfloat16


def dft_tables():
    r = np.arange(16)
    k = np.arange(256)
    twiddle = 2.0 * np.pi * np.outer(r, k) / LONS
    a = np.arange(32)
    m1 = np.concatenate([64 + a, 127 - a])
    inner = 2.0 * np.pi * (np.outer(m1, k) % 256) / 256
    cos, sin = np.cos(inner), np.sin(inner)
    both = np.stack([np.concatenate([cos, sin], 1), np.concatenate([-sin, cos], 1)])
    both = both.reshape(2, 2, 32, 512).transpose(1, 0, 2, 3).reshape(128, 512)
    both = both.astype(np.float32)
    high = both.astype(BF16)
    low = (both - high.astype(np.float32)).astype(BF16)
    return np.stack([np.cos(twiddle), np.sin(twiddle)]).astype(np.float32), high, low


def halves(x):
    high = x.astype(BF16)
    return high, (x - high.astype(F32)).astype(BF16)


def weighted(terms):
    total = None
    for weight, value in terms:
        if abs(weight) < 1e-12:
            continue
        if abs(weight - 1.0) < 1e-12:
            total = value if total is None else total + value
        elif abs(weight + 1.0) < 1e-12:
            total = -value if total is None else total - value
        else:
            total = value * weight if total is None else total + value * weight
    return total


def sixteen_point(x):
    e = [None] + [x[j] + x[16 - j] for j in range(1, 8)]
    o = [None] + [x[j] - x[16 - j] for j in range(1, 8)]
    cos = lambda t: math.cos(math.pi * t / 8)
    sin = lambda t: math.sin(math.pi * t / 8)
    base = [x[0] + x[8], x[0] - x[8]]
    re_of, im_of = [], []
    plus_e = [e[j] + e[8 - j] for j in range(1, 4)]
    less_e = [e[j] - e[8 - j] for j in range(1, 4)]
    plus_o = [o[j] + o[8 - j] for j in range(1, 4)]
    less_o = [o[j] - o[8 - j] for j in range(1, 4)]
    for r in range(9):
        fold_e, fold_o = (less_e, plus_o) if r % 2 else (plus_e, less_o)
        re_terms = [(1.0, base[r % 2])] + [(cos(j * r), fold_e[j - 1]) for j in (1, 2, 3)]
        im_terms = [(-sin(j * r), fold_o[j - 1]) for j in (1, 2, 3)]
        if r % 2:
            im_terms.append((-sin(4 * r), o[4]))
        else:
            re_terms.append((cos(4 * r), e[4]))
        re_of.append(weighted(re_terms))
        im_of.append(weighted(im_terms))
    return re_of, im_of


def dot(a, b):
    return lax.dot_general(a, b, (((1,), (0,)), ((), ())), preferred_element_type=F32)


def dot_rows(a, b):
    return lax.dot_general(a, b, (((1,), (1,)), ((), ())), preferred_element_type=F32)


def kernel(
    fields_in, legendre, pairs_in, pair_scalars, twiddle_in, high_in, low_in, out,
    fields, pairs, twiddle, inner_high, inner_low,
    staged, weights, rows, z_high, z_low, a_high, a_low, spread_pairs, chosen, ordered, arrived,
    left, part, from_core, ring_in, near_in, joined, joined_in, whole, from_far,
    leg_sem, in_sem, s1, r1, s2, r2, sa, ra, sb, rb, sc, rc, sz, rz,
):
    theta = lax.axis_index("theta")
    phi = lax.axis_index("phi")
    z, x = phi // 4, phi % 4
    y, far, core = theta // 4, (theta // 2) % 2, theta % 2
    core_mate = theta + 1 - 2 * core
    far_mate = theta + 2 - 4 * far
    up = ((y + 1) % 4) * 4 + theta % 4
    down = ((y + 3) % 4) * 4 + theta % 4

    inputs = [
        pltpu.make_async_copy(src, dst, in_sem.at[n])
        for n, (src, dst) in enumerate((
            (fields_in, fields),
            (pairs_in, pairs),
            (twiddle_in, twiddle),
            (high_in, inner_high),
            (low_in, inner_low),
        ))
    ]
    for load in inputs:
        load.start()
    loads = [
        pltpu.make_async_copy(legendre.at[pl.ds(16 * c, 16)], staged.at[pl.ds(16 * c, 16)], leg_sem.at[c])
        for c in range(4)
    ]
    for load in loads:
        load.start()

    z_order = [(z + 2) % 4, 3 - z, z + 1 - 2 * (z % 2), z]
    partners = []
    for dx in (2, 1, 3, 0):
        for step in (0, 1, 2, 3):
            if step < 3 or dx > 0:
                partners.append(z_order[step] * 4 + (x + dx) % 4)

    barrier = pltpu.get_barrier_semaphore()
    for partner in partners:
        pl.semaphore_signal(barrier, inc=1, device_id=(theta, partner), device_id_type=MESH)
    for partner in (core_mate, far_mate, up, down):
        pl.semaphore_signal(barrier, inc=1, device_id=(partner, phi), device_id_type=MESH)
    pl.semaphore_wait(barrier, 19)
    inputs[0].wait()

    def send(src, dst, send_sem, recv_sem, device):
        return pltpu.make_async_remote_copy(
            src_ref=src, dst_ref=dst, send_sem=send_sem, recv_sem=recv_sem, device_id=device, device_id_type=MESH
        )

    sent = []

    def start(*copy_args):
        copy = send(*copy_args)
        copy.start()
        sent.append(copy)
        return copy

    for h in range(2):
        lats = pl.ds(32 * h, 32)
        for n, partner in enumerate(partners):
            start(
                fields.at[partner % 8, partner // 8, lats],
                rows.at[h, phi],
                s1.at[h, n],
                r1.at[h, phi],
                (theta, partner),
            )
        rows[h, phi] = fields[phi % 8, phi // 8, lats]

    for load in inputs[1:]:
        load.wait()

    spread = jnp.broadcast_to(pairs[...].astype(F32), (128, 512))
    for block in range(4):
        at = slice(128 * block, 128 * block + 128)
        spread_pairs[at, :] = jnp.transpose(spread[:, at])
    lane = lax.broadcasted_iota(jnp.int32, (128, 128), 1)
    upper_half = lax.broadcasted_iota(jnp.int32, (16, 8, 128), 1) >= 4
    for block in range(2):
        own = spread_pairs[256 * block : 256 * block + 256, :].reshape(16, 16, 128)
        one, two = own[:, :8], own[:, 8:]
        low = jnp.where(upper_half, pltpu.roll(two, 4, 1), one).reshape(128, 128)
        top = jnp.where(upper_half, two, pltpu.roll(one, 4, 1)).reshape(128, 128)
        for turn, picked in enumerate((jnp.where(far == 0, top, low), jnp.where(far == 0, low, top))):
            for tile in range(4):
                code = (16 * (lane % 32) + (4 * tile + lane // 32)).astype(F32)
                chosen[turn, 128 * block : 128 * block + 128, 128 * tile : 128 * tile + 128] = jnp.where(
                    picked == code, 1.0, 0.0
                ).astype(BF16)

    def prepare(n, carry):
        lat, slot = 16 * (n // 4), 8 * (n % 4)
        for tile in range(9):
            lanes = slice(128 * tile, min(128 * tile + 128, PAIR_LEN))
            block = staged[pl.ds(lat, 16), pl.ds(slot, 8), lanes]
            high, low = halves(jnp.transpose(block, (1, 0, 2)))
            weights[pl.ds(slot, 8), pl.ds(lat, 16), lanes] = high
            weights[pl.ds(slot, 8), pl.ds(64 + lat, 16), lanes] = high
            weights[pl.ds(slot, 8), pl.ds(128 + lat, 16), lanes] = low
        return carry

    def outer(h):
        def body(n, carry):
            lat = pl.multiple_of(16 * (n // 2), 16)
            lanes = pl.ds(pl.multiple_of(128 * (n % 2), 128), 128)
            upper = pl.ds(pl.multiple_of(256 + 128 * (n % 2), 128), 128)
            re_of, im_of = sixteen_point([rows[h, p, pl.ds(lat, 16), lanes] for p in range(16)])
            for r in range(16):
                re = re_of[min(r, 16 - r)]
                im = im_of[min(r, 16 - r)]
                c = twiddle[0, r : r + 1, lanes]
                s = twiddle[1, r : r + 1, lanes]
                if im is None:
                    z_re, z_im = re * c, -(re * s)
                elif r <= 8:
                    z_re, z_im = re * c + im * s, im * c - re * s
                else:
                    z_re, z_im = re * c - im * s, -(im * c + re * s)
                for value, at in ((z_re, lanes), (z_im, upper)):
                    high, low = halves(value)
                    z_high[pl.ds(32 * r + lat, 16), at] = high
                    z_low[pl.ds(32 * r + lat, 16), at] = low
            return carry

        lax.fori_loop(0, 4, body, 0)

    def inner():
        for group in range(4):
            at = slice(128 * group, 128 * group + 128)
            high, low = z_high[at, :], z_low[at, :]
            both = dot_rows(inner_high[...], high) + dot_rows(inner_high[...], low) + dot_rows(inner_low[...], high)
            for j in range(4):
                lats = slice(32 * j, 32 * j + 32)
                r = 4 * group + j
                for kind, spot in ((0, r), (1, 15 - r)):
                    value = jnp.concatenate(
                        [both[64 * kind : 64 * kind + 32, lats], both[64 * kind + 32 : 64 * kind + 64, lats]], axis=1
                    )
                    high_value, low_value = halves(value)
                    a_high[32 * spot : 32 * spot + 32, 64 * kind : 64 * kind + 64] = high_value
                    a_low[32 * spot : 32 * spot + 32, 64 * kind : 64 * kind + 64] = low_value

    def put_in_order(h):
        for turn in range(2):
            picks = chosen[turn]
            ordered[h, turn] = dot(picks, a_high[...]) + dot(picks, a_low[...])

    def send_orders(h, turn):
        for n, partner in enumerate(partners):
            start(
                ordered.at[h, turn, pl.ds(pl.multiple_of(16 * partner, 16), 16)],
                arrived.at[h, turn, pl.ds(pl.multiple_of(16 * phi, 16), 16)],
                s2.at[h, turn, n],
                r2.at[h, turn, phi],
                (theta, partner),
            )
        mine = pl.ds(pl.multiple_of(16 * phi, 16), 16)
        arrived[h, turn, mine] = ordered[h, turn, mine]

    def receive_rows(h):
        for partner in partners:
            spot = rows.at[h, partner]
            send(spot, spot, s1.at[h, 0], r1.at[h, partner], (theta, partner)).wait_recv()

    for load in loads:
        load.wait()
    lax.fori_loop(0, 8, prepare, 0)
    receive_rows(0)
    outer(0)
    inner()
    put_in_order(0)
    lax.fori_loop(8, 16, prepare, 0)
    receive_rows(1)
    send_orders(0, 0)
    outer(1)
    inner()
    put_in_order(1)
    send_orders(1, 0)
    send_orders(0, 1)
    send_orders(1, 1)

    wide = lax.broadcasted_iota(jnp.int32, (64, 128), 1)
    column = lax.broadcasted_iota(jnp.int32, (8, PAIR_LEN), 1)

    def arrive(turn):
        for partner in partners:
            for h in range(2):
                spot = arrived.at[h, turn, pl.ds(pl.multiple_of(16 * partner, 16), 16)]
                send(spot, spot, s2.at[h, turn, 0], r2.at[h, turn, partner], (theta, partner)).wait_recv()

    def turn_rows(turn, e, of_core):
        def body(n, carry):
            slot = 4 * n + 2 * of_core + e
            turned = []
            for h in range(2):
                both = arrived[h, turn, pl.ds(slot, 16, stride=16), :]
                both = jnp.concatenate([both[:8] + both[8:], both[:8] - both[8:]], axis=0)
                turned.append(
                    jnp.concatenate(
                        [
                            both if (32 * h - 32 * (2 * kind + p)) % 128 == 0
                            else pltpu.roll(both, (32 * h - 32 * (2 * kind + p)) % 128, 1)
                            for p in range(2) for kind in range(2)
                        ],
                        axis=0,
                    )
                )
            value = jnp.where(wide < 32, turned[0], turned[1])
            high = value.astype(BF16).astype(F32)
            low = pltpu.roll(value - high, 64, 1)
            left[slot, :, 0:128] = jnp.where(wide < 64, high, low).astype(BF16)
            left[slot, :, 128:256] = high.astype(BF16)
            return carry

        lax.fori_loop(0, 4, body, 0, unroll=4)

    def project(turn, e, of_core):
        turn_rows(turn, e, of_core)
        z_half = far if turn else 1 - far

        def body(n, carry):
            number = 8 * n + 4 * z_half + 2 * of_core + e
            product = dot(left[4 * n + 2 * of_core + e, :, 0:192], weights[number])
            pair = pair_scalars[32 * phi + number]
            is_first = column < ORDERS - pair
            is_even = (column + jnp.where(is_first, 0, pair)) % 2 == 0
            for half in range(2):
                four = [product[32 * half + 8 * m : 32 * half + 8 * m + 8] for m in range(4)]
                lower = jnp.where(is_even, four[0], four[1])
                upper = jnp.where(is_even, four[2], four[3])
                part[turn, e, of_core, n, half] = jnp.where(is_first, lower, upper)
            return carry

        lax.fori_loop(0, 4, body, 0, unroll=4)

    y_up, y_down, y_far = (y + 1) % 4, (y + 3) % 4, (y + 2) % 4

    def to_core(turn, e):
        project(turn, e, 1 - core)
        copy = start(
            part.at[turn, e, 1 - core], from_core.at[turn, e], sa.at[turn, e], ra.at[turn, e], (core_mate, phi)
        )
        project(turn, e, core)
        return copy

    def to_ring(turn, e, copy):
        copy.wait_recv()
        part[turn, e, core] = part[turn, e, core] + from_core[turn, e]
        return [
            start(
                part.at[turn, e, core, to_y, half], dst, sb.at[turn, e, n], rb.at[turn, e, n], (device, phi)
            )
            for n, (to_y, half, dst, device) in enumerate((
                (y_far, 0, ring_in.at[turn, e, 0], up),
                (y_far, 1, ring_in.at[turn, e, 1], down),
                (y_up, 1, near_in.at[turn, e, 0], up),
                (y_down, 0, near_in.at[turn, e, 1], down),
            ))
        ]

    def join(turn, e, near):
        copies = []
        for n, (to_y, device) in enumerate(((y_up, up), (y_down, down))):
            near[n].wait_recv()
            joined[turn, e, n] = part[turn, e, core, to_y, n] + ring_in[turn, e, n]
            copies.append(
                start(
                    joined.at[turn, e, n],
                    joined_in.at[turn, e, n],
                    sc.at[turn, e, n],
                    rc.at[turn, e, n],
                    (device, phi),
                )
            )
        return copies

    def finish(turn, e, near, last):
        for copy in near[2:] + last:
            copy.wait_recv()
        for half in range(2):
            whole[turn, e, half] = (
                part[turn, e, core, y, half] + joined_in[turn, e, half] + near_in[turn, e, 1 - half]
            )
        if turn == 0:
            return start(whole.at[0, e], from_far.at[e], sz.at[e], rz.at[e], (far_mate, phi))

    arrive(0)
    core00 = to_core(0, 0)
    near00 = to_ring(0, 0, core00)
    core01 = to_core(0, 1)
    near01 = to_ring(0, 1, core01)
    arrive(1)
    core10 = to_core(1, 0)
    last00 = join(0, 0, near00)
    near10 = to_ring(1, 0, core10)
    core11 = to_core(1, 1)
    last01 = join(0, 1, near01)
    near11 = to_ring(1, 1, core11)
    far0 = finish(0, 0, near00, last00)
    last10 = join(1, 0, near10)
    far1 = finish(0, 1, near01, last01)
    last11 = join(1, 1, near11)
    finish(1, 0, near10, last10)
    finish(1, 1, near11, last11)
    for e, copy in enumerate((far0, far1)):
        copy.wait_recv()
        out[e] = whole[1, e] + from_far[e]

    for copy in sent:
        copy.wait_send()


def on_device(fields, legendre, pair_table):
    twiddle, inner_high, inner_low = dft_tables()
    vmem = pl.BlockSpec(memory_space=pltpu.VMEM)
    anywhere = pl.BlockSpec(memory_space=pltpu.HBM)
    dma = pltpu.SemaphoreType.DMA
    row = (2, 8, PAIR_LEN)
    result = pl.pallas_call(
        kernel,
        out_shape=pltpu.VMEM((2, *row), F32),
        in_specs=[
            anywhere,
            anywhere,
            anywhere,
            pl.BlockSpec(memory_space=pltpu.SMEM),
            anywhere,
            anywhere,
            anywhere,
        ],
        out_specs=vmem,
        scratch_shapes=[
            pltpu.VMEM(fields.shape, F32),
            pltpu.VMEM((1, 512), jnp.int32),
            pltpu.VMEM((2, 16, 256), F32),
            pltpu.VMEM((128, 512), BF16),
            pltpu.VMEM((128, 512), BF16),
            pltpu.VMEM((64, 32, PAIR_LEN), F32),
            pltpu.VMEM((32, 192, PAIR_LEN), BF16),
            pltpu.VMEM((2, 16, 32, 256), F32),
            pltpu.VMEM((512, 512), BF16),
            pltpu.VMEM((512, 512), BF16),
            pltpu.VMEM((512, 128), BF16),
            pltpu.VMEM((512, 128), BF16),
            pltpu.VMEM((512, 128), F32),
            pltpu.VMEM((2, 256, 512), BF16),
            pltpu.VMEM((2, 2, 256, 128), F32),
            pltpu.VMEM((2, 2, 256, 128), F32),
            pltpu.VMEM((16, 64, 256), BF16),
            pltpu.VMEM((2, 2, 2, 4, *row), F32),
            pltpu.VMEM((2, 2, 4, *row), F32),
            pltpu.VMEM((2, 2, *row), F32),
            pltpu.VMEM((2, 2, *row), F32),
            pltpu.VMEM((2, 2, *row), F32),
            pltpu.VMEM((2, 2, *row), F32),
            pltpu.VMEM((2, 2, *row), F32),
            pltpu.VMEM((2, *row), F32),
            dma((4,)),
            dma((5,)),
            dma((2, 15)), dma((2, 16)),
            dma((2, 2, 15)), dma((2, 2, 16)),
            dma((2, 2)), dma((2, 2)),
            dma((2, 2, 4)), dma((2, 2, 4)),
            dma((2, 2, 2)), dma((2, 2, 2)),
            dma((2,)), dma((2,)),
        ],
        compiler_params=pltpu.CompilerParams(
            collective_id=0, has_side_effects=True, vmem_limit_bytes=60000 * 1024
        ),
        name="harmonics",
    )(
        fields,
        legendre,
        pair_table.reshape(1, -1),
        pair_table,
        jnp.asarray(twiddle),
        jnp.asarray(inner_high),
        jnp.asarray(inner_low),
    )
    return result


def solution(mesh):
    placed = (P(None, None, "theta", "phi"), P("theta", "phi", None), P())
    return jax.shard_map(
        on_device,
        mesh=mesh,
        in_specs=placed,
        out_specs=P(("phi", "theta"), None, None, None),
        check_vma=False,
    )
```

```python
import functools
import math

import jax
import jax.numpy as jnp
import numpy as np
from jax import lax
from jax.experimental import pallas as pl
from jax.experimental.pallas import tpu as pltpu
from jax.sharding import PartitionSpec as P

LONS = 4096
ORDERS = 1024
PAIR_LEN = 1025

MESH = pl.DeviceIdType.MESH
F32 = jnp.float32
BF16 = jnp.bfloat16


def dft_tables():
    r = np.arange(16)
    k = np.arange(256)
    twiddle = 2.0 * np.pi * np.outer(r, k) / LONS
    a = np.arange(32)
    m1 = np.concatenate([64 + a, 127 - a])
    inner = 2.0 * np.pi * (np.outer(m1, k) % 256) / 256
    cos, sin = np.cos(inner), np.sin(inner)
    both = np.stack([np.concatenate([cos, sin], 1), np.concatenate([-sin, cos], 1)])
    both = both.reshape(2, 2, 32, 512).transpose(1, 0, 2, 3).reshape(128, 512)
    both = both.astype(np.float32)
    high = both.astype(BF16)
    low = (both - high.astype(np.float32)).astype(BF16)
    return np.stack([np.cos(twiddle), np.sin(twiddle)]).astype(np.float32), high, low


def halves(x):
    high = x.astype(BF16)
    return high, (x - high.astype(F32)).astype(BF16)


def weighted(terms):
    total = None
    for weight, value in terms:
        if abs(weight) < 1e-12:
            continue
        if abs(weight - 1.0) < 1e-12:
            total = value if total is None else total + value
        elif abs(weight + 1.0) < 1e-12:
            total = -value if total is None else total - value
        else:
            total = value * weight if total is None else total + value * weight
    return total


def sixteen_point(x):
    e = [None] + [x[j] + x[16 - j] for j in range(1, 8)]
    o = [None] + [x[j] - x[16 - j] for j in range(1, 8)]
    cos = lambda t: math.cos(math.pi * t / 8)
    sin = lambda t: math.sin(math.pi * t / 8)
    base = [x[0] + x[8], x[0] - x[8]]
    re_of, im_of = [], []
    plus_e = [e[j] + e[8 - j] for j in range(1, 4)]
    less_e = [e[j] - e[8 - j] for j in range(1, 4)]
    plus_o = [o[j] + o[8 - j] for j in range(1, 4)]
    less_o = [o[j] - o[8 - j] for j in range(1, 4)]
    for r in range(9):
        fold_e, fold_o = (less_e, plus_o) if r % 2 else (plus_e, less_o)
        re_terms = [(1.0, base[r % 2])] + [(cos(j * r), fold_e[j - 1]) for j in (1, 2, 3)]
        im_terms = [(-sin(j * r), fold_o[j - 1]) for j in (1, 2, 3)]
        if r % 2:
            im_terms.append((-sin(4 * r), o[4]))
        else:
            re_terms.append((cos(4 * r), e[4]))
        re_of.append(weighted(re_terms))
        im_of.append(weighted(im_terms))
    return re_of, im_of


def dot(a, b):
    return lax.dot_general(a, b, (((1,), (0,)), ((), ())), preferred_element_type=F32)


def dot_rows(a, b):
    return lax.dot_general(a, b, (((1,), (1,)), ((), ())), preferred_element_type=F32)


def kernel(
    fields_in, legendre, pairs_in, pair_scalars, twiddle_in, high_in, low_in, out,
    fields, pairs, twiddle, inner_high, inner_low,
    staged, weights, rows, z_high, z_low, a_high, a_low, spread_pairs, chosen, ordered, arrived,
    left, part, from_core, ring_in, near_in, joined, joined_in, whole, from_far,
    leg_sem, in_sem, s1, r1, s2, r2, sa, ra, sb, rb, sc, rc, sz, rz,
):
    theta = lax.axis_index("theta")
    phi = lax.axis_index("phi")
    z, x = phi // 4, phi % 4
    y, far, core = theta // 4, (theta // 2) % 2, theta % 2
    core_mate = theta + 1 - 2 * core
    far_mate = theta + 2 - 4 * far
    up = ((y + 1) % 4) * 4 + theta % 4
    down = ((y + 3) % 4) * 4 + theta % 4

    inputs = [
        pltpu.make_async_copy(src, dst, in_sem.at[n])
        for n, (src, dst) in enumerate((
            (fields_in, fields),
            (pairs_in, pairs),
            (twiddle_in, twiddle),
            (high_in, inner_high),
            (low_in, inner_low),
        ))
    ]
    for load in inputs:
        load.start()
    loads = [
        pltpu.make_async_copy(legendre.at[pl.ds(16 * c, 16)], staged.at[pl.ds(16 * c, 16)], leg_sem.at[c])
        for c in range(4)
    ]
    for load in loads:
        load.start()

    z_order = [(z + 2) % 4, 3 - z, z + 1 - 2 * (z % 2), z]
    partners = []
    for step in (0, 1, 2, 3):
        for dx in (2, 1, 3, 0):
            if step < 3 or dx > 0:
                partners.append(z_order[step] * 4 + (x + dx) % 4)

    barrier = pltpu.get_barrier_semaphore()
    for partner in partners:
        pl.semaphore_signal(barrier, inc=1, device_id=(theta, partner), device_id_type=MESH)
    for partner in (core_mate, far_mate, up, down):
        pl.semaphore_signal(barrier, inc=1, device_id=(partner, phi), device_id_type=MESH)
    pl.semaphore_wait(barrier, 19)
    inputs[0].wait()

    def send(src, dst, send_sem, recv_sem, device):
        return pltpu.make_async_remote_copy(
            src_ref=src, dst_ref=dst, send_sem=send_sem, recv_sem=recv_sem, device_id=device, device_id_type=MESH
        )

    sent = []

    def start(*copy_args):
        copy = send(*copy_args)
        copy.start()
        sent.append(copy)
        return copy

    for h in range(2):
        lats = pl.ds(32 * h, 32)
        for n, partner in enumerate(partners):
            start(
                fields.at[partner % 8, partner // 8, lats],
                rows.at[h, phi],
                s1.at[h, n],
                r1.at[h, phi],
                (theta, partner),
            )
        rows[h, phi] = fields[phi % 8, phi // 8, lats]

    for load in inputs[1:]:
        load.wait()

    spread = jnp.broadcast_to(pairs[...].astype(F32), (128, 512))
    for block in range(4):
        at = slice(128 * block, 128 * block + 128)
        spread_pairs[at, :] = jnp.transpose(spread[:, at])
    lane = lax.broadcasted_iota(jnp.int32, (128, 128), 1)
    upper_half = lax.broadcasted_iota(jnp.int32, (16, 8, 128), 1) >= 4
    for block in range(2):
        own = spread_pairs[256 * block : 256 * block + 256, :].reshape(16, 16, 128)
        one, two = own[:, :8], own[:, 8:]
        low = jnp.where(upper_half, pltpu.roll(two, 4, 1), one).reshape(128, 128)
        top = jnp.where(upper_half, two, pltpu.roll(one, 4, 1)).reshape(128, 128)
        for turn, picked in enumerate((jnp.where(far == 0, top, low), jnp.where(far == 0, low, top))):
            for tile in range(4):
                code = (16 * (lane % 32) + (4 * tile + lane // 32)).astype(F32)
                chosen[turn, 128 * block : 128 * block + 128, 128 * tile : 128 * tile + 128] = jnp.where(
                    picked == code, 1.0, 0.0
                ).astype(BF16)

    def prepare(n, carry):
        lat, slot = 16 * (n // 4), 8 * (n % 4)
        for tile in range(9):
            lanes = slice(128 * tile, min(128 * tile + 128, PAIR_LEN))
            block = staged[pl.ds(lat, 16), pl.ds(slot, 8), lanes]
            high, low = halves(jnp.transpose(block, (1, 0, 2)))
            weights[pl.ds(slot, 8), pl.ds(lat, 16), lanes] = high
            weights[pl.ds(slot, 8), pl.ds(64 + lat, 16), lanes] = high
            weights[pl.ds(slot, 8), pl.ds(128 + lat, 16), lanes] = low
        return carry

    def outer(h):
        def body(n, carry):
            lat = pl.multiple_of(16 * (n // 2), 16)
            lanes = pl.ds(pl.multiple_of(128 * (n % 2), 128), 128)
            upper = pl.ds(pl.multiple_of(256 + 128 * (n % 2), 128), 128)
            re_of, im_of = sixteen_point([rows[h, p, pl.ds(lat, 16), lanes] for p in range(16)])
            for r in range(16):
                re = re_of[min(r, 16 - r)]
                im = im_of[min(r, 16 - r)]
                c = twiddle[0, r : r + 1, lanes]
                s = twiddle[1, r : r + 1, lanes]
                if im is None:
                    z_re, z_im = re * c, -(re * s)
                elif r <= 8:
                    z_re, z_im = re * c + im * s, im * c - re * s
                else:
                    z_re, z_im = re * c - im * s, -(im * c + re * s)
                for value, at in ((z_re, lanes), (z_im, upper)):
                    high, low = halves(value)
                    z_high[pl.ds(32 * r + lat, 16), at] = high
                    z_low[pl.ds(32 * r + lat, 16), at] = low
            return carry

        lax.fori_loop(0, 4, body, 0)

    def inner():
        for group in range(4):
            at = slice(128 * group, 128 * group + 128)
            high, low = z_high[at, :], z_low[at, :]
            both = dot_rows(inner_high[...], high) + dot_rows(inner_high[...], low) + dot_rows(inner_low[...], high)
            for j in range(4):
                lats = slice(32 * j, 32 * j + 32)
                r = 4 * group + j
                for kind, spot in ((0, r), (1, 15 - r)):
                    value = jnp.concatenate(
                        [both[64 * kind : 64 * kind + 32, lats], both[64 * kind + 32 : 64 * kind + 64, lats]], axis=1
                    )
                    high_value, low_value = halves(value)
                    a_high[32 * spot : 32 * spot + 32, 64 * kind : 64 * kind + 64] = high_value
                    a_low[32 * spot : 32 * spot + 32, 64 * kind : 64 * kind + 64] = low_value

    def put_in_order(h):
        for turn in range(2):
            picks = chosen[turn]
            ordered[h, turn] = dot(picks, a_high[...]) + dot(picks, a_low[...])

    def send_orders(h, turn):
        for n, partner in enumerate(partners):
            start(
                ordered.at[h, turn, pl.ds(pl.multiple_of(16 * partner, 16), 16)],
                arrived.at[h, turn, pl.ds(pl.multiple_of(16 * phi, 16), 16)],
                s2.at[h, turn, n],
                r2.at[h, turn, phi],
                (theta, partner),
            )
        mine = pl.ds(pl.multiple_of(16 * phi, 16), 16)
        arrived[h, turn, mine] = ordered[h, turn, mine]

    def receive_rows(h):
        for partner in partners:
            spot = rows.at[h, partner]
            send(spot, spot, s1.at[h, 0], r1.at[h, partner], (theta, partner)).wait_recv()

    for load in loads:
        load.wait()
    lax.fori_loop(0, 8, prepare, 0)
    receive_rows(0)
    outer(0)
    inner()
    put_in_order(0)
    lax.fori_loop(8, 16, prepare, 0)
    receive_rows(1)
    send_orders(0, 0)
    outer(1)
    inner()
    put_in_order(1)
    send_orders(1, 0)
    send_orders(0, 1)
    send_orders(1, 1)

    wide = lax.broadcasted_iota(jnp.int32, (64, 128), 1)
    column = lax.broadcasted_iota(jnp.int32, (8, PAIR_LEN), 1)

    def arrive(turn):
        for partner in partners:
            for h in range(2):
                spot = arrived.at[h, turn, pl.ds(pl.multiple_of(16 * partner, 16), 16)]
                send(spot, spot, s2.at[h, turn, 0], r2.at[h, turn, partner], (theta, partner)).wait_recv()

    def turn_rows(turn, e, of_core):
        def body(n, carry):
            slot = 4 * n + 2 * of_core + e
            turned = []
            for h in range(2):
                both = arrived[h, turn, pl.ds(slot, 16, stride=16), :]
                both = jnp.concatenate([both[:8] + both[8:], both[:8] - both[8:]], axis=0)
                turned.append(
                    jnp.concatenate(
                        [
                            both if (32 * h - 32 * (2 * kind + p)) % 128 == 0
                            else pltpu.roll(both, (32 * h - 32 * (2 * kind + p)) % 128, 1)
                            for p in range(2) for kind in range(2)
                        ],
                        axis=0,
                    )
                )
            value = jnp.where(wide < 32, turned[0], turned[1])
            high = value.astype(BF16).astype(F32)
            low = pltpu.roll(value - high, 64, 1)
            left[slot, :, 0:128] = jnp.where(wide < 64, high, low).astype(BF16)
            left[slot, :, 128:256] = high.astype(BF16)
            return carry

        lax.fori_loop(0, 4, body, 0, unroll=4)

    def project(turn, e, of_core):
        turn_rows(turn, e, of_core)
        z_half = far if turn else 1 - far

        def body(n, carry):
            number = 8 * n + 4 * z_half + 2 * of_core + e
            product = dot(left[4 * n + 2 * of_core + e, :, 0:192], weights[number])
            pair = pair_scalars[32 * phi + number]
            is_first = column < ORDERS - pair
            is_even = (column + jnp.where(is_first, 0, pair)) % 2 == 0
            for half in range(2):
                four = [product[32 * half + 8 * m : 32 * half + 8 * m + 8] for m in range(4)]
                lower = jnp.where(is_even, four[0], four[1])
                upper = jnp.where(is_even, four[2], four[3])
                part[turn, e, of_core, n, half] = jnp.where(is_first, lower, upper)
            return carry

        lax.fori_loop(0, 4, body, 0, unroll=4)

    y_up, y_down, y_far = (y + 1) % 4, (y + 3) % 4, (y + 2) % 4

    def to_core(turn, e):
        project(turn, e, 1 - core)
        copy = start(
            part.at[turn, e, 1 - core], from_core.at[turn, e], sa.at[turn, e], ra.at[turn, e], (core_mate, phi)
        )
        project(turn, e, core)
        return copy

    def to_ring(turn, e, copy):
        copy.wait_recv()
        part[turn, e, core] = part[turn, e, core] + from_core[turn, e]
        return [
            start(
                part.at[turn, e, core, to_y, half], dst, sb.at[turn, e, n], rb.at[turn, e, n], (device, phi)
            )
            for n, (to_y, half, dst, device) in enumerate((
                (y_far, 0, ring_in.at[turn, e, 0], up),
                (y_far, 1, ring_in.at[turn, e, 1], down),
                (y_up, 1, near_in.at[turn, e, 0], up),
                (y_down, 0, near_in.at[turn, e, 1], down),
            ))
        ]

    def join(turn, e, near):
        copies = []
        for n, (to_y, device) in enumerate(((y_up, up), (y_down, down))):
            near[n].wait_recv()
            joined[turn, e, n] = part[turn, e, core, to_y, n] + ring_in[turn, e, n]
            copies.append(
                start(
                    joined.at[turn, e, n],
                    joined_in.at[turn, e, n],
                    sc.at[turn, e, n],
                    rc.at[turn, e, n],
                    (device, phi),
                )
            )
        return copies

    def finish(turn, e, near, last):
        for copy in near[2:] + last:
            copy.wait_recv()
        for half in range(2):
            whole[turn, e, half] = (
                part[turn, e, core, y, half] + joined_in[turn, e, half] + near_in[turn, e, 1 - half]
            )
        if turn == 0:
            return start(whole.at[0, e], from_far.at[e], sz.at[e], rz.at[e], (far_mate, phi))

    arrive(0)
    core00 = to_core(0, 0)
    near00 = to_ring(0, 0, core00)
    core01 = to_core(0, 1)
    near01 = to_ring(0, 1, core01)
    arrive(1)
    core10 = to_core(1, 0)
    last00 = join(0, 0, near00)
    near10 = to_ring(1, 0, core10)
    core11 = to_core(1, 1)
    last01 = join(0, 1, near01)
    near11 = to_ring(1, 1, core11)
    far0 = finish(0, 0, near00, last00)
    last10 = join(1, 0, near10)
    far1 = finish(0, 1, near01, last01)
    last11 = join(1, 1, near11)
    finish(1, 0, near10, last10)
    finish(1, 1, near11, last11)
    for e, copy in enumerate((far0, far1)):
        copy.wait_recv()
        out[e] = whole[1, e] + from_far[e]

    for copy in sent:
        copy.wait_send()


def on_device(fields, legendre, pair_table):
    twiddle, inner_high, inner_low = dft_tables()
    vmem = pl.BlockSpec(memory_space=pltpu.VMEM)
    anywhere = pl.BlockSpec(memory_space=pltpu.HBM)
    dma = pltpu.SemaphoreType.DMA
    row = (2, 8, PAIR_LEN)
    result = pl.pallas_call(
        kernel,
        out_shape=pltpu.VMEM((2, *row), F32),
        in_specs=[
            anywhere,
            anywhere,
            anywhere,
            pl.BlockSpec(memory_space=pltpu.SMEM),
            anywhere,
            anywhere,
            anywhere,
        ],
        out_specs=vmem,
        scratch_shapes=[
            pltpu.VMEM(fields.shape, F32),
            pltpu.VMEM((1, 512), jnp.int32),
            pltpu.VMEM((2, 16, 256), F32),
            pltpu.VMEM((128, 512), BF16),
            pltpu.VMEM((128, 512), BF16),
            pltpu.VMEM((64, 32, PAIR_LEN), F32),
            pltpu.VMEM((32, 192, PAIR_LEN), BF16),
            pltpu.VMEM((2, 16, 32, 256), F32),
            pltpu.VMEM((512, 512), BF16),
            pltpu.VMEM((512, 512), BF16),
            pltpu.VMEM((512, 128), BF16),
            pltpu.VMEM((512, 128), BF16),
            pltpu.VMEM((512, 128), F32),
            pltpu.VMEM((2, 256, 512), BF16),
            pltpu.VMEM((2, 2, 256, 128), F32),
            pltpu.VMEM((2, 2, 256, 128), F32),
            pltpu.VMEM((16, 64, 256), BF16),
            pltpu.VMEM((2, 2, 2, 4, *row), F32),
            pltpu.VMEM((2, 2, 4, *row), F32),
            pltpu.VMEM((2, 2, *row), F32),
            pltpu.VMEM((2, 2, *row), F32),
            pltpu.VMEM((2, 2, *row), F32),
            pltpu.VMEM((2, 2, *row), F32),
            pltpu.VMEM((2, 2, *row), F32),
            pltpu.VMEM((2, *row), F32),
            dma((4,)),
            dma((5,)),
            dma((2, 15)), dma((2, 16)),
            dma((2, 2, 15)), dma((2, 2, 16)),
            dma((2, 2)), dma((2, 2)),
            dma((2, 2, 4)), dma((2, 2, 4)),
            dma((2, 2, 2)), dma((2, 2, 2)),
            dma((2,)), dma((2,)),
        ],
        compiler_params=pltpu.CompilerParams(
            collective_id=0, has_side_effects=True, vmem_limit_bytes=60000 * 1024
        ),
        name="harmonics",
    )(
        fields,
        legendre,
        pair_table.reshape(1, -1),
        pair_table,
        jnp.asarray(twiddle),
        jnp.asarray(inner_high),
        jnp.asarray(inner_low),
    )
    return result


def solution(mesh):
    placed = (P(None, None, "theta", "phi"), P("theta", "phi", None), P())
    return jax.shard_map(
        on_device,
        mesh=mesh,
        in_specs=placed,
        out_specs=P(("phi", "theta"), None, None, None),
        check_vma=False,
    )
```
